32 devices in a mesh: dp: 2 (over core), seq: 8 (over z, x), mp: 2 (over y).
Axes of the slice: x: 2, y: 2, z: 4, core: 2. Of those that a mesh axis runs over, the one named last changes fastest.
Arguments:
- queries: bfloat16 [4, 1024, 4096], P('dp', 'seq', 'mp'), may hold values from -6 to 6
- vision: bfloat16 [4, 640, 4096], P('dp', 'seq'), may hold values from -6 to 6
- key_weight: bfloat16 [4096, 1024], P(None, 'mp'), may hold values from -0.09375 to 0.09375
- value_weight: bfloat16 [4096, 1024], P(None, 'mp'), may hold values from -0.09375 to 0.09375
- query_gain: float32 [128], replicated, may hold values from 0.6 to 6
- key_gain: float32 [128], replicated, may hold values from 0.6 to 6
- out_grad: bfloat16 [4, 1024, 4096], P('dp', 'seq', 'mp'), may hold values from -6 to 6
- tile_count: int32 [4], P('dp'), may hold values from 1 to 4, as said below
Outputs:
- query_grad: bfloat16 [4, 1024, 4096], P('dp', 'seq', 'mp')
- vision_grad: bfloat16 [4, 640, 4096], P('dp', 'seq', 'mp')
- key_weight_grad: float32 [4096, 1024], P(None, 'mp')
- value_weight_grad: float32 [4096, 1024], P(None, 'mp')
The draws below stay inside these ranges and needn't reach their ends.
Inputs may be any that keep to these rules, and one draw needn't show every extreme that they name: The live vision tokens of sample s are its first tile_count[s] * 160; some sample has 4 tiles and some other sample has 1.
All inputs are finite; a program needn't handle non-finite values.
Results may differ from the reference program's by a relative error of at most 0.03.
The reference program's roundings to bfloat16 on the way (of `keys`, `values`, `normed`, `probs_b`, `attn`, `dscores`, `key_grad` and `value_grad`) count: a program that leaves them out, or rounds other values in their place, can miss the bound.
Values may be sent and summed in bfloat16 or wider, within the bound.
A program may use at most 128 MiB of HBM per device.

```python
import jax
import jax.numpy as jnp
from jax import lax

D = 4096
HEADS = 32
KV_HEADS = 8
HEAD_DIM = 128
MAX_TILES = 4
SAMPLES = 4
TXT = 1024
VIS = 640
TILE_TOK = 160


def vision_field(key):
    drawn = jax.random.normal(jax.random.fold_in(key, 7001), (SAMPLES, VIS, D), jnp.float32)
    return jnp.clip(drawn, -6.0, 6.0)


def key_matrix(key):
    drawn = jax.random.normal(jax.random.fold_in(key, 7002), (D, KV_HEADS * HEAD_DIM), jnp.float32)
    return jnp.clip(drawn, -6.0, 6.0) * D ** (-0.5)


def draw_vision(key, part):
    return vision_field(key).astype(jnp.bfloat16)


def draw_key_weight(key, part):
    return key_matrix(key).astype(jnp.bfloat16)


def draw_queries(key, part):
    drawn = jax.random.normal(jax.random.fold_in(key, 7003), (SAMPLES, TXT, HEADS * HEAD_DIM), jnp.float32)
    drawn = jnp.clip(drawn, -6.0, 6.0)
    return drawn.astype(jnp.bfloat16)


def draw_query_gain(key, part):
    inner = jax.random.fold_in(key, 7005)
    return jax.random.uniform(inner, (HEAD_DIM,), jnp.float32, 0.6, 1.4)


def draw_key_gain(key, part):
    inner = jax.random.fold_in(key, 7006)
    return jax.random.uniform(inner, (HEAD_DIM,), jnp.float32, 0.6, 1.4)


def draw_tile_count(key, part):
    counts = jax.random.randint(jax.random.fold_in(key, 7101), (SAMPLES,), 1, MAX_TILES + 1, dtype=jnp.int32)
    full_at = jax.random.randint(jax.random.fold_in(key, 7102), (), 0, SAMPLES, dtype=jnp.int32)
    step_to = jax.random.randint(jax.random.fold_in(key, 7103), (), 1, SAMPLES, dtype=jnp.int32)
    single_at = (full_at + step_to) % SAMPLES
    counts = counts.at[full_at].set(MAX_TILES)
    counts = counts.at[single_at].set(1)
    return counts.astype(jnp.int32)


def steps_of(stream_key, extent, pieces, smallest, top_value):
    def one(dim, shards_of):
        heights = jax.random.uniform(jax.random.fold_in(jax.random.fold_in(stream_key, 6), dim), (shards_of,), jnp.float32, smallest / len(pieces), top_value / len(pieces))
        return jnp.repeat(jnp.exp(heights), extent[dim] // shards_of).reshape((-1,) + (1,) * (len(extent) - dim - 1))

    level = one(*pieces[0])
    for cut in pieces[1:]:
        level = level * one(*cut)
    return level


def noise(own_key, dims, scale, bound, split=(), kind=jnp.bfloat16):
    values = jax.random.normal(own_key, dims, jnp.float32) * scale
    if len(split) > 0:
        values = steps_of(own_key, dims, split, -0.22, 0.18) * values
    return jnp.clip(values, min=-bound, max=bound).astype(kind)


def setup_inputs(seed: int = 0) -> dict:
    key_of = jax.random.split(jax.random.key(seed), 9)
    queries = draw_queries(jax.random.fold_in(key_of[8], 71), 0)
    vision = draw_vision(jax.random.fold_in(key_of[8], 71), 0)
    key_weight = draw_key_weight(jax.random.fold_in(key_of[8], 71), 0)
    value_weight = noise(key_of[3], (D, KV_HEADS * HEAD_DIM), D ** -0.5, 0.09375, ((1, 2),))
    query_gain = draw_query_gain(jax.random.fold_in(key_of[8], 71), 0)
    key_gain = draw_key_gain(jax.random.fold_in(key_of[8], 71), 0)
    out_grad = noise(key_of[6], (SAMPLES, TXT, HEADS * HEAD_DIM), 1.0, 6.0, ((0, 2), (1, 8), (2, 2)))
    tile_count = draw_tile_count(jax.random.fold_in(key_of[8], 71), 0)
    return {"queries": queries, "vision": vision, "key_weight": key_weight, "value_weight": value_weight, "query_gain": query_gain, "key_gain": key_gain, "out_grad": out_grad, "tile_count": tile_count}


EPS = 1e-05
NEG = -1e+30

def norm_apply(raw, gain):
    inverse = lax.rsqrt(lax.optimization_barrier(jnp.mean(raw * raw, axis=-1, keepdims=True)) + EPS)
    return (raw * inverse * gain, inverse)

def norm_back(raw, inverse, gain, upstream):
    weighted = upstream * gain
    return inverse * weighted - raw * inverse * inverse * inverse * lax.optimization_barrier(jnp.mean(weighted * raw, axis=-1, keepdims=True))

def sample_grads(queries_one, vision_one, out_one, tiles_one, key_weight, value_weight, query_gain, key_gain):
    group_size = HEADS // KV_HEADS
    score_scale = HEAD_DIM ** (-0.5)
    key_cols = key_weight.reshape(D, KV_HEADS, HEAD_DIM).transpose(1, 0, 2)
    value_cols = value_weight.reshape(D, KV_HEADS, HEAD_DIM).transpose(1, 0, 2)
    query_heads = queries_one.reshape(TXT, KV_HEADS, group_size, HEAD_DIM).transpose(1, 0, 2, 3)
    out_heads = out_one.reshape(TXT, KV_HEADS, group_size, HEAD_DIM).transpose(1, 0, 2, 3)
    live_keys = jnp.arange(VIS, dtype=jnp.int32) < tiles_one * TILE_TOK

    def one_group(vision_total, inputs):
        key_col, value_col, query_group, out_group = inputs
        key_raw = jnp.dot(vision_one, key_col, preferred_element_type=jnp.float32)
        key_normed, key_inverse = norm_apply(key_raw, key_gain)
        keys = key_normed.astype(jnp.bfloat16)
        values = jnp.dot(vision_one, value_col, preferred_element_type=jnp.float32).astype(jnp.bfloat16)
        query_raw = query_group.astype(jnp.float32)
        query_normed, query_inverse = norm_apply(query_raw, query_gain)
        normed = query_normed.astype(jnp.bfloat16)
        normed_wide = normed.astype(jnp.float32)
        keys_wide = keys.astype(jnp.float32)
        values_wide = values.astype(jnp.float32)
        out_wide = out_group.astype(jnp.float32)
        scores = jnp.einsum('tgd,jd->gtj', normed_wide, keys_wide) * score_scale
        scores = jnp.where(live_keys[None, None, :], scores, NEG)
        row_top = lax.optimization_barrier(jnp.max(scores, axis=-1, keepdims=True))
        expo = jnp.exp(scores - row_top)
        probs = expo / lax.optimization_barrier(jnp.sum(expo, axis=-1, keepdims=True))
        probs_b = probs.astype(jnp.bfloat16)
        probs_wide = probs_b.astype(jnp.float32)
        attn = jnp.einsum('gtj,jd->tgd', probs_wide, values_wide).astype(jnp.bfloat16)
        delta = lax.optimization_barrier(jnp.sum(out_wide * attn.astype(jnp.float32), axis=-1))
        dprobs = jnp.einsum('tgd,jd->gtj', out_wide, values_wide)
        dscores = (probs * (dprobs - delta.T[:, :, None])).astype(jnp.bfloat16)
        dscores_wide = dscores.astype(jnp.float32)
        dnormed = jnp.einsum('gtj,jd->tgd', dscores_wide, keys_wide) * score_scale
        dkeys = jnp.einsum('gtj,tgd->jd', dscores_wide, normed_wide) * score_scale
        dvalues = jnp.einsum('gtj,tgd->jd', probs_wide, out_wide)
        query_part = norm_back(query_raw, query_inverse, query_gain, dnormed).astype(jnp.bfloat16)
        key_grad = norm_back(key_raw, key_inverse, key_gain, dkeys).astype(jnp.bfloat16)
        value_grad = dvalues.astype(jnp.bfloat16)
        key_weight_part = jnp.dot(vision_one.T, key_grad, preferred_element_type=jnp.float32)
        value_weight_part = jnp.dot(vision_one.T, value_grad, preferred_element_type=jnp.float32)
        vision_term = jnp.dot(key_grad, key_col.T, preferred_element_type=jnp.float32)
        vision_term = vision_term + jnp.dot(value_grad, value_col.T, preferred_element_type=jnp.float32)
        return (vision_total + vision_term, (query_part, key_weight_part, value_weight_part))
    start_total = jnp.zeros((VIS, D), jnp.float32)
    vision_total, stacked = lax.scan(one_group, start_total, (key_cols, value_cols, query_heads, out_heads))
    query_parts, key_parts, value_parts = stacked
    query_grad = query_parts.transpose(1, 0, 2, 3).reshape(TXT, HEADS * HEAD_DIM)
    key_weight_part = key_parts.transpose(1, 0, 2).reshape(D, KV_HEADS * HEAD_DIM)
    value_weight_part = value_parts.transpose(1, 0, 2).reshape(D, KV_HEADS * HEAD_DIM)
    return (query_grad, vision_total.astype(jnp.bfloat16), key_weight_part, value_weight_part)

def reference(queries, vision, key_weight, value_weight, query_gain, key_gain, out_grad, tile_count):
    query_list = []
    vision_list = []
    key_weight_grad = jnp.zeros((D, KV_HEADS * HEAD_DIM), jnp.float32)
    value_weight_grad = jnp.zeros((D, KV_HEADS * HEAD_DIM), jnp.float32)
    for sample_at in range(SAMPLES):
        query_part, vision_part, key_part, value_part = sample_grads(queries[sample_at], vision[sample_at], out_grad[sample_at], tile_count[sample_at], key_weight, value_weight, query_gain, key_gain)
        query_list.append(query_part)
        vision_list.append(vision_part)
        key_weight_grad = key_weight_grad + key_part
        value_weight_grad = value_weight_grad + value_part
    return (jnp.stack(query_list), jnp.stack(vision_list), key_weight_grad, value_weight_grad)
```

```python
import functools

import jax
import jax.numpy as jnp
from jax import lax
from jax.experimental import pallas as pl
from jax.experimental.pallas import tpu as pltpu
from jax.sharding import PartitionSpec as P

MAX_TILES = 4
EPS = 1e-05
NEG = -1e30
MESH = pl.DeviceIdType.MESH
VMEM = pltpu.VMEM
F32 = jnp.float32
BF16 = jnp.bfloat16


def norm_back(raw, inverse, gain, upstream):
    weighted = upstream * gain
    return inverse * weighted - raw * inverse * inverse * inverse * jnp.mean(
        weighted * raw, axis=-1, keepdims=True
    )


def inverse_of(raw):
    return lax.rsqrt(jnp.mean(raw * raw, axis=-1, keepdims=True) + EPS)


def seq_of(place, n):
    half = place // (n // 2)
    along = place + half * (n - 1 - 2 * place)
    return 2 * along + half


def place_of(index, n):
    side = index % 2
    along = index // 2
    return along + side * (n - 1 - 2 * along)


def ring(n):
    here = lax.axis_index("seq")
    place = place_of(here, n)
    nexts = (seq_of((place + 1) % n, n), seq_of((place + n - 1) % n, n))
    return here, place, nexts


def greet(devices):
    barrier = pltpu.get_barrier_semaphore()
    for device in devices:
        pl.semaphore_signal(barrier, inc=1, device_id=device, device_id_type=MESH)
    pl.semaphore_wait(barrier, len(devices))


def run_ring(n, pairs, sources, outs, sems, prepare=None, jobs=(), kept=True):
    send_sem, recv_sem, pair_send, pair_recv = sems
    here, place, nexts = ring(n)
    lane = lax.axis_index("dp") if pairs > 1 else 0
    chunks = sources[0].shape[0]
    others = [(lane + shift) % pairs for shift in range(1, pairs)]
    ring_copies, pair_copies = {}, []
    jobs = list(jobs)

    def pass_on(way, step, chunk):
        origin = seq_of((place + n - step) % n if way == 0 else (place + step) % n, n)
        target = outs[way].at[lane, chunk, origin] if kept else outs[way].at[chunk, origin]
        block = sources[way].at[chunk] if step == 0 else target
        if step > 0:
            ring_copies[way, step - 1, chunk].wait_recv()
        if step < n - 1:
            copy = pltpu.make_async_remote_copy(
                src_ref=block,
                dst_ref=target,
                send_sem=send_sem.at[way, step, chunk],
                recv_sem=recv_sem.at[way, step, chunk],
                device_id={"seq": nexts[way]},
                device_id_type=MESH,
            )
            copy.start()
            ring_copies[way, step, chunk] = copy
        for at, other in enumerate(others):
            copy = pltpu.make_async_remote_copy(
                src_ref=block,
                dst_ref=target,
                send_sem=pair_send.at[way, step, chunk, at],
                recv_sem=pair_recv.at[way, step, chunk, at],
                device_id={"dp": other},
                device_id_type=MESH,
            )
            copy.start()
            pair_copies.append(copy)

    for way in range(2):
        if prepare is not None:
            prepare(way)
        for chunk in range(chunks):
            pass_on(way, 0, chunk)
    for way in range(2):
        for chunk in range(chunks):
            if kept:
                outs[way][lane, chunk, here] = sources[way][chunk]
            else:
                outs[way][chunk, here] = sources[way][chunk]
    for step in range(1, n):
        for chunk in range(chunks):
            if jobs:
                jobs.pop(0)()
            for way in range(2):
                pass_on(way, step, chunk)
    for job in jobs:
        job()
    for copy in ring_copies.values():
        copy.wait_send()
    for copy in pair_copies:
        copy.wait_send()
        copy.wait_recv()


def ring_sems(n, pairs, chunks):
    return [
        pltpu.SemaphoreType.DMA((2, n, chunks)),
        pltpu.SemaphoreType.DMA((2, n, chunks)),
        pltpu.SemaphoreType.DMA((2, n, chunks, max(pairs - 1, 1))),
        pltpu.SemaphoreType.DMA((2, n, chunks, max(pairs - 1, 1))),
    ]


def greet_ring(n, pairs, mates=()):
    nexts = ring(n)[2]
    lane = lax.axis_index("dp")
    others = [{"dp": (lane + shift) % pairs} for shift in range(1, pairs)]
    greet([{"seq": nexts[0]}, {"seq": nexts[1]}] + others + list(mates))


def size_of(*arrays):
    return sum(array.size * array.dtype.itemsize for array in arrays)


def limit_of(*arrays):
    return size_of(*arrays) + 4 * 1024 * 1024


def cost_of(sent):
    return pl.CostEstimate(flops=25_000_000_000, bytes_accessed=sent, transcendentals=0)


WEIGHT_CUTS = 4


def project_kernel(sizes, vision_hbm, key_hbm, value_hbm, gain_ref, keys_out, values_out, raw_out,
                   vision, key_weight, value_weight, own_keys, own_values, load_sem, *sems):
    pairs, n, heads_cut = sizes
    samples, rows, width = vision.shape
    columns = key_weight.shape[1]
    head_dim = gain_ref.shape[1]
    depth = width // WEIGHT_CUTS

    loads = [pltpu.make_async_copy(vision_hbm, vision, load_sem.at[0])]
    for at, (source, held) in enumerate(((key_hbm, key_weight), (value_hbm, value_weight))):
        for cut in range(WEIGHT_CUTS):
            span = pl.ds(cut * depth, depth)
            loads.append(
                pltpu.make_async_copy(
                    source.at[span], held.at[span], load_sem.at[1 + at * WEIGHT_CUTS + cut]
                )
            )
    for load in loads:
        load.start()
    greet_ring(n, 1)
    loads[0].wait()

    def product(at, weight, cut, total):
        loads[1 + at * WEIGHT_CUTS + cut].wait()
        left = vision[:, :, cut * depth : (cut + 1) * depth].reshape(samples * rows, depth)
        part = jnp.dot(left, weight[cut * depth : (cut + 1) * depth], preferred_element_type=F32)
        return part if total is None else total + part

    state = {}

    def prepare(way):
        if way == 0:
            raw = None
            for cut in range(WEIGHT_CUTS):
                raw = product(0, key_weight, cut, raw)
            for at in range(columns // head_dim):
                span = slice(at * head_dim, (at + 1) * head_dim)
                head = raw[:, span]
                normed = (head * inverse_of(head) * gain_ref[...]).astype(BF16)
                raw_out[:, :, span] = head.reshape(samples, rows, head_dim)
                own_keys[:, :, span] = normed.reshape(samples, rows, head_dim)
            state["values"] = product(1, value_weight, 0, None)
            return
        total = state["values"]
        for cut in range(1, WEIGHT_CUTS):
            total = product(1, value_weight, cut, total)
        own_values[...] = total.astype(BF16).reshape(samples, rows, columns)

    run_ring(n, 1, (own_keys, own_values), (keys_out, values_out), sems, prepare, kept=False)


def project(sizes, vision, key_weight, value_weight, gain):
    pairs, n, heads_cut = sizes
    samples, rows, width = vision.shape
    columns = key_weight.shape[1]
    gathered = jax.ShapeDtypeStruct((samples, n, rows, columns), BF16)
    raw = jax.ShapeDtypeStruct((samples, rows, columns), F32)
    sent = 2 * samples * (n - 1) * rows * columns * 2
    dma = pltpu.SemaphoreType.DMA
    own = pltpu.VMEM((samples, rows, columns), BF16)
    return pl.pallas_call(
        functools.partial(project_kernel, sizes),
        out_shape=(gathered, gathered, raw),
        in_specs=[pl.BlockSpec(memory_space=pltpu.HBM)] * 3 + [pl.BlockSpec(memory_space=VMEM)],
        out_specs=(pl.BlockSpec(memory_space=VMEM),) * 3,
        scratch_shapes=[
            pltpu.VMEM(vision.shape, BF16),
            pltpu.VMEM(key_weight.shape, BF16),
            pltpu.VMEM(value_weight.shape, BF16),
            own,
            own,
            dma((1 + 2 * WEIGHT_CUTS,)),
        ]
        + ring_sems(n, 1, samples),
        compiler_params=pltpu.CompilerParams(
            collective_id=1,
            has_side_effects=True,
            vmem_limit_bytes=60 * 1024 * 1024,
        ),
        cost_estimate=cost_of(sent),
        name="project_gather",
    )(vision, key_weight, value_weight, gain)


def spread(n, pairs, chunks, source, target, sems, ready, landed, jobs=()):
    send_sem, recv_sem, pair_send, pair_recv = sems
    here, place, nexts = ring(n)
    lane = lax.axis_index("dp")
    ring_copies, pair_copies = {}, {}
    jobs = list(jobs)

    def origin_of(way, step):
        return seq_of((place + n - step) % n if way == 0 else (place + step) % n, n)

    def pass_on(way, step, chunk):
        target_ref = target(way, chunk, lane, origin_of(way, step))
        block = source(way, chunk) if step == 0 else target_ref
        if step > 0:
            ring_copies[way, step - 1, chunk].wait_recv()
        if step < n - 1:
            copy = pltpu.make_async_remote_copy(
                src_ref=block,
                dst_ref=target_ref,
                send_sem=send_sem.at[way, step, chunk],
                recv_sem=recv_sem.at[way, step, chunk],
                device_id={"seq": nexts[way]},
                device_id_type=MESH,
            )
            copy.start()
            ring_copies[way, step, chunk] = copy
        for at in range(pairs - 1):
            copy = pltpu.make_async_remote_copy(
                src_ref=block,
                dst_ref=target_ref,
                send_sem=pair_send.at[way, step, chunk, at],
                recv_sem=pair_recv.at[way, step, chunk, at],
                device_id={"dp": (lane + 1 + at) % pairs},
                device_id_type=MESH,
            )
            copy.start()
            pair_copies[way, step, chunk, at] = copy

    def settle(step, chunk):
        for way in range(2):
            for at in range(pairs - 1):
                pair_copies[way, step, chunk, at].wait_recv()
                landed(way, chunk, (lane + pairs - 1 - at) % pairs, origin_of(way, step))

    for chunk in range(chunks):
        ready(chunk)
        for way in range(2):
            pass_on(way, 0, chunk)
    for step in range(1, n):
        for chunk in range(chunks):
            if jobs:
                jobs.pop(0)()
            for way in range(2):
                pass_on(way, step, chunk)
            for way in range(2):
                landed(way, chunk, lane, origin_of(way, step))
            settle(step - 1, chunk)
    for job in jobs:
        job()
    for chunk in range(chunks):
        settle(n - 1, chunk)
    for copy in [*ring_copies.values(), *pair_copies.values()]:
        copy.wait_send()


def finish_kernel(sizes, tile, key_ref, value_ref, columns_ref, key_weight, value_weight, vision_out, key_out,
                  value_out, leaving, arrived, total, every, mine, parts, leave_sem, arrive_sem, *sems):
    pairs, n, heads_cut = sizes
    lane, here, me = lax.axis_index("dp"), lax.axis_index("seq"), lax.axis_index("mp")
    mates = [(me + shift) % heads_cut for shift in range(1, heads_cut)]
    greet_ring(n, pairs, [{"mp": mate} for mate in mates])
    grads = (key_ref, value_ref)
    share = total.shape[1]
    samples, rows, columns = key_ref.shape
    each = samples // 2
    tokens = pairs * samples * n * rows
    tiles = share // tile
    copies = []

    def compute(owner, at, store):
        span = pl.ds(pl.multiple_of(owner * share + at * tile, tile), tile)
        part = None
        for ref, weight in ((key_ref, key_weight), (value_ref, value_weight)):
            left = ref[...].reshape(total.shape[0], columns)
            term = lax.dot_general(
                left, weight[span, :], (((1,), (1,)), ((), ())), preferred_element_type=F32
            )
            part = term if part is None else part + term
        store(part)

    def leave(at):
        copy = pltpu.make_async_remote_copy(
            src_ref=leaving.at[at],
            dst_ref=arrived.at[at],
            send_sem=leave_sem.at[at],
            recv_sem=arrive_sem.at[at],
            device_id={"mp": mates[at]},
            device_id_type=MESH,
        )
        copy.start()
        copies.append(copy)

    jobs = []
    waiting = None
    for turn, owner in enumerate(mates + [me]):
        for at in range(tiles):
            span = slice(at * tile, (at + 1) * tile)

            def job(turn=turn, owner=owner, at=at, span=span, due=waiting):
                def store(part):
                    if turn < len(mates):
                        leaving[turn, :, span] = part.astype(BF16)
                    else:
                        total[:, span] = part

                compute(owner, at, store)
                if due is not None:
                    leave(due)

            jobs.append(job)
            waiting = None
        waiting = turn

    def half_of(way):
        return pl.ds(way * each, each)

    def keep_own(chunk):
        every[chunk, lane, :, here] = grads[chunk][...]

    def nothing(*_):
        pass

    spread(
        n,
        pairs,
        2,
        lambda way, chunk: grads[chunk].at[half_of(way)],
        lambda way, chunk, whose, origin: every.at[chunk, whose, half_of(way), origin],
        sems[:4],
        keep_own,
        nothing,
        jobs,
    )

    outs = (key_out, value_out)

    def product(chunk):
        grad = lax.dot_general(
            columns_ref[...].reshape(tokens, columns_ref.shape[-1]),
            every[chunk].reshape(tokens, columns),
            (((0,), (0,)), ((), ())),
            preferred_element_type=F32,
        ).astype(BF16)
        mine[chunk] = grad.reshape(mine.shape[1:])

    def widen(way, chunk, whose, origin):
        outs[chunk][whose, origin, way] = parts[chunk, whose, origin, way].astype(F32)

    def widen_own():
        for chunk in range(2):
            outs[chunk][lane, here] = mine[chunk].astype(F32)

    def finish_vision():
        result = total[...]
        for at, copy in enumerate(copies):
            copy.wait()
            result = result + arrived[at].astype(F32)
        vision_out[...] = result.astype(BF16)

    spread(
        n,
        pairs,
        2,
        lambda way, chunk: mine.at[chunk, way],
        lambda way, chunk, whose, origin: parts.at[chunk, whose, origin, way],
        sems[4:],
        product,
        widen,
        [finish_vision, widen_own],
    )


def finish(sizes, key_grad, value_grad, column_vision, key_weight, value_weight):
    pairs, n, heads_cut = sizes
    samples, rows, columns = key_grad.shape
    width = key_weight.shape[0]
    share = width // heads_cut
    tile = 512 if share % 512 == 0 else share
    shard = column_vision.shape[-1]
    vision = jax.ShapeDtypeStruct((samples * rows, share), BF16)
    moved = pltpu.VMEM((max(heads_cut - 1, 1), samples * rows, share), BF16)
    grad = jax.ShapeDtypeStruct((pairs, n, 2, shard // 2, columns), F32)
    sent = 2 * samples * (n - 1) * rows * columns * 2 + 2 * (n - 1) * shard * columns * 2
    dma = pltpu.SemaphoreType.DMA
    return pl.pallas_call(
        functools.partial(finish_kernel, sizes, tile),
        out_shape=(vision, grad, grad),
        in_specs=[pl.BlockSpec(memory_space=VMEM)] * 5,
        out_specs=(pl.BlockSpec(memory_space=VMEM),) * 3,
        scratch_shapes=[
            moved,
            moved,
            pltpu.VMEM(vision.shape, F32),
            pltpu.VMEM((2, pairs, samples, n, rows, columns), BF16),
            pltpu.VMEM((2, 2, shard // 2, columns), BF16),
            pltpu.VMEM((2, pairs, n, 2, shard // 2, columns), BF16),
            dma((max(heads_cut - 1, 1),)),
            dma((max(heads_cut - 1, 1),)),
        ]
        + ring_sems(n, pairs, 2)
        + ring_sems(n, pairs, 2),
        compiler_params=pltpu.CompilerParams(
            collective_id=3, has_side_effects=True, vmem_limit_bytes=FINISH_LIMIT
        ),
        cost_estimate=cost_of(sent),
        name="finish",
    )(key_grad, value_grad, column_vision, key_weight, value_weight)


FINISH_LIMIT = 22 * 1024 * 1024


def scatter_kernel(n, groups, head_dim, key_ref, value_ref, raw_ref, gain_ref, half_ref, key_out, value_out,
                   columns_out, held, send_sem, recv_sem, own_sem, mate_send, mate_recv):
    parts = (key_ref, value_ref)
    here, place, nexts = ring(n)
    chunks = key_ref.shape[0]
    me = lax.axis_index("mp")
    seat = me % groups
    mates = [me - seat + (seat + shift) % groups for shift in range(1, groups)]
    greet([{"seq": nexts[0]}, {"seq": nexts[1]}] + [{"mp": mate} for mate in mates])

    def copy_of(way, step, chunk, block):
        return pltpu.make_async_remote_copy(
            src_ref=block,
            dst_ref=held.at[way, step, chunk],
            send_sem=send_sem.at[way, step, chunk],
            recv_sem=recv_sem.at[way, step, chunk],
            device_id={"seq": nexts[way]},
            device_id_type=MESH,
        )

    def dest_of(way, step):
        if way == 0:
            return seq_of((place + 2 * n - 1 - step) % n, n)
        return seq_of((place + 1 + step) % n, n)

    copies = {}
    for chunk in range(chunks):
        for way in range(2):
            copy = copy_of(way, 0, chunk, parts[way].at[chunk, dest_of(way, 0)])
            copy.start()
            copies[way, 0, chunk] = copy
    moved = []
    for cut in range(half_ref.shape[0]):
        for pair in range(half_ref.shape[1]):
            for at in range(half_ref.shape[2]):
                block = half_ref.at[cut, pair, at]
                target = columns_out.at[cut, pair, seat if groups > 1 else at]
                moved.append(pltpu.make_async_copy(block, target, own_sem.at[cut, pair, at]))
                for turn, mate in enumerate(mates):
                    moved.append(
                        pltpu.make_async_remote_copy(
                            src_ref=block,
                            dst_ref=target,
                            send_sem=mate_send.at[cut, pair, turn],
                            recv_sem=mate_recv.at[cut, pair, turn],
                            device_id={"mp": mate},
                            device_id_type=MESH,
                        )
                    )
    for copy in moved:
        copy.start()
    for step in range(1, n):
        for chunk in range(chunks):
            for way in range(2):
                copies[way, step - 1, chunk].wait_recv()
                own = parts[way][chunk, dest_of(way, step)].astype(F32)
                total = held[way, step - 1, chunk].astype(F32) + own
                if step < n - 1:
                    held[way, step - 1, chunk] = total.astype(BF16)
                elif way == 1:
                    value_out[chunk] = total.astype(BF16)
                else:
                    gain = gain_ref[...]
                    for at in range(total.shape[1] // head_dim):
                        cut = slice(at * head_dim, (at + 1) * head_dim)
                        raw = raw_ref[chunk, :, cut]
                        grad = norm_back(raw, inverse_of(raw), gain, total[:, cut])
                        key_out[chunk, :, cut] = grad.astype(BF16)
            if step < n - 1:
                for way in range(2):
                    copy = copy_of(way, step, chunk, held.at[way, step - 1, chunk])
                    copy.start()
                    copies[way, step, chunk] = copy
    for copy in copies.values():
        copy.wait_send()
    for copy in moved:
        copy.wait()


def ring_scatter(sizes, key_part, value_part, key_raw, gain, half, number):
    chunks, n, rows, columns = key_part.shape
    groups = chunks if sizes[2] % chunks == 0 else 1
    cuts, pairs, each = half.shape[:3]
    full = jax.ShapeDtypeStruct((cuts, pairs, chunks) + half.shape[3:], BF16)
    dma = pltpu.SemaphoreType.DMA
    out = jax.ShapeDtypeStruct((chunks, rows, columns), BF16)
    sent = 2 * chunks * (n - 1) * rows * columns * 2
    return pl.pallas_call(
        functools.partial(scatter_kernel, n, groups, gain.shape[1]),
        out_shape=(out, out, full),
        in_specs=[pl.BlockSpec(memory_space=VMEM)] * 5,
        out_specs=(pl.BlockSpec(memory_space=VMEM),) * 3,
        scratch_shapes=[
            pltpu.VMEM((2, n - 1, chunks, rows, columns), BF16),
            dma((2, n - 1, chunks)),
            dma((2, n - 1, chunks)),
            dma((cuts, pairs, each)),
            dma((cuts, pairs, max(groups - 1, 1))),
            dma((cuts, pairs, max(groups - 1, 1))),
        ],
        compiler_params=pltpu.CompilerParams(
            collective_id=number,
            has_side_effects=True,
            vmem_limit_bytes=limit_of(key_part, value_part, key_part, value_part, key_raw, out, out, half, full),
        ),
        cost_estimate=cost_of(sent),
        name="ring_scatter",
    )(key_part, value_part, key_raw, gain, half)


def exchange(sizes, groups, vision, columns_out, push_send, push_recv, own_sem):
    pairs, n, _ = sizes
    chunks, each, shard = columns_out.shape[0], columns_out.shape[2], columns_out.shape[-1]
    lane, here, me = lax.axis_index("dp"), lax.axis_index("seq"), lax.axis_index("mp")
    peers = [((lane + shift // n) % pairs, (here + shift % n) % n) for shift in range(1, pairs * n)]
    own, pushes = [], []
    for chunk in range(chunks):
        for at in range(each):
            sample = me % groups if groups > 1 else at

            def columns_of(pair, seat, chunk=chunk, sample=sample):
                start = ((pair * chunks + chunk) * n + seat) * shard
                return vision.at[sample, :, pl.ds(pl.multiple_of(start, shard), shard)]

            target = columns_out.at[chunk, lane, at, here]
            own.append(pltpu.make_async_copy(columns_of(lane, here), target, own_sem.at[chunk, at]))
            for shift, peer in enumerate(peers):
                pushes.append(
                    pltpu.make_async_remote_copy(
                        src_ref=columns_of(*peer),
                        dst_ref=target,
                        send_sem=push_send.at[chunk, at, shift],
                        recv_sem=push_recv.at[chunk, at, shift],
                        device_id={"dp": peer[0], "seq": peer[1]},
                        device_id_type=MESH,
                    )
                )
    return peers, own + pushes


def attention_kernel(sizes, groups, group, tile_tokens, tiles_ref, query_ref, grad_ref, key_ref, value_ref,
                     gain_ref, vision, query_out, key_out, value_out, columns_out, *sems):
    at_sample, at_head = pl.program_id(0), pl.program_id(1)
    heads = pl.num_programs(1)
    turn = at_sample * heads + at_head

    @pl.when(turn == 0)
    def _():
        peers, copies = exchange(sizes, groups, vision, columns_out, *sems)
        greet([{"dp": peer[0], "seq": peer[1]} for peer in peers])
        for copy in copies:
            copy.start()

    text_rows = query_ref.shape[1]
    head_dim = key_ref.shape[2]
    scale = head_dim ** (-0.5)
    live = tiles_ref[pl.program_id(0)] * tile_tokens

    def stacked(ref):
        return jnp.concatenate(
            [ref[0, :, at * head_dim : (at + 1) * head_dim] for at in range(group)], axis=0
        )

    def mul(left, right, dims):
        return lax.dot_general(left, right, (dims, ((), ())), preferred_element_type=F32)

    raw = stacked(query_ref).astype(F32)
    outs = stacked(grad_ref)
    gain = gain_ref[...]
    inverse = inverse_of(raw)
    normed = (raw * inverse * gain).astype(BF16)
    keys = key_ref[0]
    values = value_ref[0]
    scores = mul(normed, keys, ((1,), (1,))) * scale
    token = lax.broadcasted_iota(jnp.int32, scores.shape, 1)
    scores = jnp.where(token < live, scores, NEG)
    expo = jnp.exp(scores - jnp.max(scores, axis=-1, keepdims=True))
    probs = expo * (1.0 / jnp.sum(expo, axis=-1, keepdims=True))
    probs_b = probs.astype(BF16)
    attn = mul(probs_b, values, ((1,), (0,))).astype(BF16)
    delta = jnp.sum(outs.astype(F32) * attn.astype(F32), axis=-1, keepdims=True)
    dprobs = mul(outs, values, ((1,), (1,)))
    dscores = (probs * (dprobs - delta)).astype(BF16)
    value_out[0] = mul(probs_b, outs, ((0,), (0,))).astype(BF16)
    key_out[0] = (mul(dscores, normed, ((0,), (0,))) * scale).astype(BF16)
    dnormed = mul(dscores, keys, ((1,), (0,))) * scale
    back = norm_back(raw, inverse, gain, dnormed).astype(BF16)
    for at in range(group):
        query_out[0, :, at * head_dim : (at + 1) * head_dim] = back[at * text_rows : (at + 1) * text_rows]

    @pl.when(turn == pl.num_programs(0) * heads - 1)
    def _():
        for copy in exchange(sizes, groups, vision, columns_out, *sems)[1]:
            copy.wait()


def attention(sizes, tiles, queries, out_grad, keys, values, gain, vision):
    pairs, n, heads_cut = sizes
    rows, width = vision.shape[1:]
    samples, text_rows, query_width = queries.shape
    tokens, key_width = keys.shape[1:]
    head_dim = gain.shape[1]
    heads = key_width // head_dim
    group = query_width // key_width
    wide = pl.BlockSpec((1, text_rows, group * head_dim), lambda s, h: (s, 0, h))
    tall = pl.BlockSpec((1, tokens, head_dim), lambda s, h: (s, 0, h))
    flops = samples * query_width * text_rows * tokens * 10
    part = jax.ShapeDtypeStruct((samples, tokens, key_width), BF16)
    groups = samples if heads_cut % samples == 0 else 1
    each = 1 if groups > 1 else samples
    chunks = 1
    cut = jax.ShapeDtypeStruct((chunks, pairs, each, n, rows, width // (pairs * chunks * n)), BF16)
    dma = pltpu.SemaphoreType.DMA
    return pl.pallas_call(
        functools.partial(attention_kernel, sizes, groups, group, tokens // MAX_TILES),
        grid=(samples, heads),
        out_shape=(jax.ShapeDtypeStruct(queries.shape, BF16), part, part, cut),
        in_specs=[
            pl.BlockSpec(memory_space=pltpu.SMEM),
            wide,
            wide,
            tall,
            tall,
            pl.BlockSpec((1, head_dim), lambda s, h: (0, 0)),
            pl.BlockSpec(memory_space=pltpu.HBM),
        ],
        out_specs=(wide, tall, tall, pl.BlockSpec(memory_space=pltpu.HBM)),
        scratch_shapes=[
            dma((chunks, each, pairs * n)),
            dma((chunks, each, pairs * n)),
            dma((chunks, each)),
        ],
        compiler_params=pltpu.CompilerParams(
            collective_id=5, has_side_effects=True, vmem_limit_bytes=40 * 1024 * 1024
        ),
        cost_estimate=pl.CostEstimate(flops=flops, bytes_accessed=8_000_000, transcendentals=0),
        name="attention",
    )(tiles, queries, out_grad, keys, values, gain, vision)


def local(sizes, queries, vision, key_weight, value_weight, query_gain, key_gain, out_grad, tile_count):
    pairs, n, heads_cut = sizes
    samples, rows, model_width = vision.shape
    columns = key_weight.shape[1]
    keys_all, values_all, key_raw = project(
        sizes, vision, key_weight, value_weight, key_gain[None]
    )
    query_grad, key_part, value_part, half = attention(
        sizes,
        tile_count,
        queries,
        out_grad,
        keys_all.reshape(samples, n * rows, columns),
        values_all.reshape(samples, n * rows, columns),
        query_gain[None],
        vision,
    )
    key_grad, value_grad, column_vision = ring_scatter(
        sizes,
        key_part.reshape(samples, n, rows, columns),
        value_part.reshape(samples, n, rows, columns),
        key_raw,
        key_gain[None],
        half,
        2,
    )
    vision_grad, key_weight_grad, value_weight_grad = finish(
        sizes, key_grad, value_grad, column_vision[0], key_weight, value_weight
    )
    return (
        query_grad,
        vision_grad.reshape(samples, rows, -1),
        key_weight_grad.reshape(model_width, columns),
        value_weight_grad.reshape(model_width, columns),
    )


def solution(mesh):
    sizes = (mesh.shape["dp"], mesh.shape["seq"], mesh.shape["mp"])
    in_specs = (
        P("dp", "seq", "mp"),
        P("dp", "seq", None),
        P(None, "mp"),
        P(None, "mp"),
        P(),
        P(),
        P("dp", "seq", "mp"),
        P("dp"),
    )
    out_specs = (P("dp", "seq", "mp"), P("dp", "seq", "mp"), P(None, "mp"), P(None, "mp"))
    return jax.shard_map(
        functools.partial(local, sizes), mesh=mesh, in_specs=in_specs, out_specs=out_specs, check_vma=False
    )
```

```python
import functools

import jax
import jax.numpy as jnp
from jax import lax
from jax.experimental import pallas as pl
from jax.experimental.pallas import tpu as pltpu
from jax.sharding import PartitionSpec as P

MAX_TILES = 4
EPS = 1e-05
NEG = -1e30
CUTS = 4
MESH = pl.DeviceIdType.MESH
VMEM = pltpu.VMEM
F32 = jnp.float32
BF16 = jnp.bfloat16


def norm_back(raw, inverse, gain, upstream):
    weighted = upstream * gain
    return inverse * weighted - raw * inverse * inverse * inverse * jnp.mean(
        weighted * raw, axis=-1, keepdims=True
    )


def inverse_of(raw):
    return lax.rsqrt(jnp.mean(raw * raw, axis=-1, keepdims=True) + EPS)


def seq_of(place, n):
    half = place // (n // 2)
    along = place + half * (n - 1 - 2 * place)
    return 2 * along + half


def place_of(index, n):
    side = index % 2
    along = index // 2
    return along + side * (n - 1 - 2 * along)


def greet(devices):
    barrier = pltpu.get_barrier_semaphore()
    for device in devices:
        pl.semaphore_signal(barrier, inc=1, device_id=device, device_id_type=MESH)
    pl.semaphore_wait(barrier, len(devices))


def mul(left, right, dims):
    return lax.dot_general(left, right, (dims, ((), ())), preferred_element_type=F32)


def remote(source, target, send_sem, recv_sem, device):
    return pltpu.make_async_remote_copy(
        src_ref=source,
        dst_ref=target,
        send_sem=send_sem,
        recv_sem=recv_sem,
        device_id=device,
        device_id_type=MESH,
    )


class Ring:
    def __init__(self, n):
        self.n = n
        self.here = lax.axis_index("seq")
        self.place = place_of(self.here, n)
        self.nexts = (seq_of((self.place + 1) % n, n), seq_of((self.place + n - 1) % n, n))

    def origin(self, way, step):
        n, place = self.n, self.place
        return seq_of((place + n - step) % n if way == 0 else (place + step) % n, n)

    def dest(self, way, step):
        n, place = self.n, self.place
        return seq_of((place + 2 * n - 1 - step) % n if way == 0 else (place + 1 + step) % n, n)


def is_first(step):
    return isinstance(step, int) and step == 0


class Gather:
    def __init__(self, ring, pairs, chunks, source, target, sems, landed=None):
        self.ring, self.pairs, self.chunks = ring, pairs, chunks
        self.source, self.target, self.sems, self.landed = source, target, sems, landed
        self.lane = lax.axis_index("dp")

    def ring_copy(self, way, chunk, step):
        target = self.target(way, chunk, self.lane, self.ring.origin(way, step))
        block = self.source(way, chunk) if is_first(step) else target
        send, recv = self.sems[0].at[way, step, chunk], self.sems[1].at[way, step, chunk]
        return remote(block, target, send, recv, {"seq": self.ring.nexts[way]})

    def pair_copy(self, way, chunk, step, at):
        target = self.target(way, chunk, self.lane, self.ring.origin(way, step))
        block = self.source(way, chunk) if is_first(step) else target
        send, recv = self.sems[2].at[way, step, chunk, at], self.sems[3].at[way, step, chunk, at]
        return remote(block, target, send, recv, {"dp": (self.lane + 1 + at) % self.pairs})

    def start(self, way, chunk, step, last=False):
        if not last:
            self.ring_copy(way, chunk, step).start()
        for at in range(self.pairs - 1):
            self.pair_copy(way, chunk, step, at).start()

    def step(self, chunk, step):
        last = isinstance(step, int) and step == self.ring.n - 1
        for way in range(2):
            self.ring_copy(way, chunk, step - 1).wait_recv()
            self.start(way, chunk, step, last)
        if self.landed is not None:
            for way in range(2):
                self.landed(way, chunk, self.lane, self.ring.origin(way, step))
        self.settle(chunk, step - 1)

    def settle(self, chunk, step):
        for way in range(2):
            for at in range(self.pairs - 1):
                self.pair_copy(way, chunk, step, at).wait_recv()
                if self.landed is not None:
                    whose = (self.lane + self.pairs - 1 - at) % self.pairs
                    self.landed(way, chunk, whose, self.ring.origin(way, step))

    def drain(self):
        n = self.ring.n
        for chunk in range(self.chunks):
            for way in range(2):
                for step in range(n):
                    if step < n - 1:
                        self.ring_copy(way, chunk, step).wait_send()
                    for at in range(self.pairs - 1):
                        self.pair_copy(way, chunk, step, at).wait_send()


def whole_kernel(sizes, group, tile_tokens, tile, tiles_hbm, query_hbm, vision_hbm, key_hbm, value_hbm, query_gain_hbm,
                 key_gain_hbm, grad_hbm, query_out, vision_out, key_weight, value_weight, tiles_ref, query_gain, key_gain, queries,
                 out_grad, vision, own, raw_keys,
                 gathered, parts, held, columns, grads, leaving, arrived, total, every, mine, load_sem, own_sem,
                 push_send, push_recv, mate_send, mate_recv, scatter_send, scatter_recv, leave_sem, arrive_sem, *sems):
    pairs, n, heads_cut = sizes
    ring = Ring(n)
    weights = (key_weight, value_weight)
    here, lane, me = ring.here, lax.axis_index("dp"), lax.axis_index("mp")
    samples, rows, width = vision.shape
    heads, _, text_rows, wide = queries.shape
    head_dim = key_gain.shape[1]
    model_columns = heads * head_dim
    tokens = n * rows
    scale = head_dim ** (-0.5)
    depth = width // CUTS
    shard = columns.shape[-1]
    groups = samples if heads_cut % samples == 0 else 1

    loads = [pltpu.make_async_copy(vision_hbm, vision, load_sem.at[0])]
    for at, source in enumerate((key_hbm, value_hbm)):
        for cut in range(CUTS):
            span = pl.ds(cut * depth, depth)
            loads.append(
                pltpu.make_async_copy(source.at[span], weights[at].at[span], load_sem.at[1 + at * CUTS + cut])
            )
    later = [(key_gain_hbm, key_gain), (query_gain_hbm, query_gain), (tiles_hbm, tiles_ref)]
    for head in range(heads):
        for source, target in ((query_hbm, queries), (grad_hbm, out_grad)):
            later.append((source.at[:, :, head * wide : (head + 1) * wide], target.at[head]))
    for at, (source, target) in enumerate(later):
        loads.append(pltpu.make_async_copy(source, target, load_sem.at[1 + 2 * CUTS + at]))
    for load in loads:
        load.start()

    peers = [((lane + shift // n) % pairs, (here + shift % n) % n) for shift in range(1, pairs * n)]
    mates = [(me + shift) % heads_cut for shift in range(1, heads_cut)]
    greet([{"dp": peer[0], "seq": peer[1]} for peer in peers] + [{"mp": mate} for mate in mates])
    loads[0].wait()

    seat = me % groups
    kept = [seat] if groups > 1 else list(range(samples))

    def columns_of(sample, pair, index, held_in=None):
        held_in = vision if held_in is None else held_in
        return held_in.at[sample, :, pl.ds(pl.multiple_of((pair * n + index) * shard, shard), shard)]

    pushes = [
        remote(
            columns_of(sample, *peer),
            columns.at[lane, sample, here],
            push_send.at[at, shift],
            push_recv.at[at, shift],
            {"dp": peer[0], "seq": peer[1]},
        )
        for at, sample in enumerate(kept)
        for shift, peer in enumerate(peers)
    ]
    for copy in pushes:
        copy.start()
    mine_here = [
        pltpu.make_async_copy(
            columns_of(sample, lane, here, vision_hbm), columns.at[lane, sample, here], own_sem.at[at]
        )
        for at, sample in enumerate(kept)
    ]
    for copy in mine_here:
        copy.start()
    swaps = [
        remote(
            columns.at[pair, seat],
            columns.at[pair, seat],
            mate_send.at[pair, at],
            mate_recv.at[pair, at],
            {"mp": me - seat + (seat + 1 + at) % groups},
        )
        for pair in range(pairs)
        for at in range(groups - 1)
    ]

    gather = Gather(
        ring,
        1,
        samples,
        lambda way, chunk: own.at[way, chunk],
        lambda way, chunk, whose, origin: gathered.at[way, chunk, origin],
        sems[:4],
    )

    def project(at):
        product = None
        for cut in range(CUTS):
            loads[1 + at * CUTS + cut].wait()
            left = vision[:, :, cut * depth : (cut + 1) * depth].reshape(samples * rows, depth)
            part = jnp.dot(left, weights[at][cut * depth : (cut + 1) * depth], preferred_element_type=F32)
            product = part if product is None else product + part
        return product

    product = project(0)
    loads[1 + 2 * CUTS].wait()
    for at in range(heads):
        span = slice(at * head_dim, (at + 1) * head_dim)
        head = product[:, span]
        normed = (head * inverse_of(head) * key_gain[...]).astype(BF16)
        raw_keys[:, at] = head.reshape(samples, rows, head_dim)
        own[0, :, at] = normed.reshape(samples, rows, head_dim)
    gather.start(0, 0, 0)
    product = project(1).astype(BF16)
    for at in range(heads):
        own[1, :, at] = product[:, at * head_dim : (at + 1) * head_dim].reshape(samples, rows, head_dim)
    gather.start(1, 0, 0)
    for at in range(2):
        gathered[at, :, here] = own[at]

    lag = heads
    for step in range(1, n):
        gather.step(0, step)
        if step == lag:
            for way in range(2):
                gather.start(way, 1, 0)
        if lag < step < n - 1:
            gather.step(1, step - lag)

    def attend(sample, head):
        live = tiles_ref[:, sample : sample + 1] * tile_tokens

        def stacked(ref):
            cuts = [ref[head, sample, :, at * head_dim : (at + 1) * head_dim] for at in range(group)]
            return jnp.concatenate(cuts, axis=0)

        raw = stacked(queries).astype(F32)
        outs = stacked(out_grad)
        gain = query_gain[...]
        inverse = inverse_of(raw)
        normed = (raw * inverse * gain).astype(BF16)
        keys = gathered[0, sample, :, head].reshape(tokens, head_dim)
        values = gathered[1, sample, :, head].reshape(tokens, head_dim)
        scores = mul(normed, keys, ((1,), (1,))) * scale
        token = lax.broadcasted_iota(jnp.int32, scores.shape, 1)
        scores = jnp.where(token < live, scores, NEG)
        expo = jnp.exp(scores - jnp.max(scores, axis=-1, keepdims=True))
        probs = expo * (1.0 / jnp.sum(expo, axis=-1, keepdims=True))
        probs_b = probs.astype(BF16)
        attn = mul(probs_b, values, ((1,), (0,))).astype(BF16)
        delta = jnp.sum(outs.astype(F32) * attn.astype(F32), axis=-1, keepdims=True)
        dprobs = mul(outs, values, ((1,), (1,)))
        dscores = (probs * (dprobs - delta)).astype(BF16)
        value_part = mul(probs_b, outs, ((0,), (0,))).astype(BF16)
        key_part = (mul(dscores, normed, ((0,), (0,))) * scale).astype(BF16)
        parts[0, sample, :, head] = key_part.reshape(n, rows, head_dim)
        parts[1, sample, :, head] = value_part.reshape(n, rows, head_dim)
        dnormed = mul(dscores, keys, ((1,), (0,))) * scale
        back = norm_back(raw, inverse, gain, dnormed).astype(BF16)
        for at in range(group):
            cut = slice(at * head_dim, (at + 1) * head_dim)
            query_out[head, sample, :, cut] = back[at * text_rows : (at + 1) * text_rows]

    def scatter_copy(way, chunk, step, block=None):
        block = held.at[way, chunk, step] if block is None else block
        send, recv = scatter_send.at[way, step, chunk], scatter_recv.at[way, step, chunk]
        return remote(block, held.at[way, chunk, step], send, recv, {"seq": ring.nexts[way]})

    def scatter_start(chunk):
        for way in range(2):
            scatter_copy(way, chunk, 0, parts.at[way, chunk, ring.dest(way, 0)]).start()

    def scatter_sum(way, chunk, step):
        scatter_copy(way, chunk, step - 1).wait_recv()
        return held[way, chunk, step - 1].astype(F32) + parts[way, chunk, ring.dest(way, step)].astype(F32)

    def scatter_step(chunk, step):
        for way in range(2):
            held[way, chunk, step - 1] = scatter_sum(way, chunk, step).astype(BF16)
            scatter_copy(way, chunk, step, held.at[way, chunk, step - 1]).start()

    def scatter_last(chunk):
        summed = scatter_sum(0, chunk, n - 1)
        values = scatter_sum(1, chunk, n - 1)
        gain = key_gain[...]
        for at in range(heads):
            cut = slice(at * head_dim, (at + 1) * head_dim)
            raw = raw_keys[chunk, at]
            grads[0, chunk, :, cut] = norm_back(raw, inverse_of(raw), gain, summed[at]).astype(BF16)
            grads[1, chunk, :, cut] = values[at].astype(BF16)

    for load in loads[2 + 2 * CUTS :]:
        load.wait()

    def first_sample(head, carry):
        gather.step(1, n - 1 - lag + head)
        attend(0, head)
        return carry

    lax.fori_loop(0, heads, first_sample, 0)
    scatter_start(0)
    gather.step(1, n - 1)
    for copy in pushes:
        copy.wait_recv()
    for copy in mine_here:
        copy.wait()
    for copy in swaps:
        copy.start()

    def second_sample(head, carry):
        scatter_step(0, head + 1)
        attend(1, head)
        return carry

    lax.fori_loop(0, heads, second_sample, 0)
    scatter_start(1)

    spread = Gather(
        ring,
        pairs,
        samples,
        lambda way, chunk: grads.at[way, chunk],
        lambda way, chunk, whose, origin: every.at[way, whose, chunk, origin],
        sems[4:8],
    )
    for step in range(heads + 1, n):
        if step < n - 1:
            scatter_step(0, step)
        else:
            scatter_last(0)
            for way in range(2):
                spread.start(way, 0, 0)
        scatter_step(1, step - heads)
    for step in range(1, heads):
        spread.step(0, step)
        scatter_step(1, n - 1 - heads + step)
    spread.step(0, heads)
    scatter_last(1)
    for way in range(2):
        spread.start(way, 1, 0)
        every[way, lane, :, here] = grads[way]

    share = total.shape[1]
    tiles = share // tile
    copies = []

    def vision_part(owner, at):
        span = pl.ds(pl.multiple_of(owner * share + at * tile, tile), tile)
        part = None
        for kind in range(2):
            left = grads[kind].reshape(samples * rows, model_columns)
            term = mul(left, weights[kind][span, :], ((1,), (1,)))
            part = term if part is None else part + term
        return part

    def leave(at):
        copy = remote(leaving.at[at], arrived.at[at], leave_sem.at[at], arrive_sem.at[at], {"mp": mates[at]})
        copy.start()
        copies.append(copy)

    jobs = []
    for turn, owner in enumerate(mates + [me]):
        for at in range(tiles):

            def job(turn=turn, owner=owner, at=at):
                span = slice(at * tile, (at + 1) * tile)
                part = vision_part(owner, at)
                if turn == len(mates):
                    total[:, span] = part
                    return
                leaving[turn, :, span] = part.astype(BF16)
                if at == tiles - 1:
                    leave(turn)

            jobs.append(job)

    plan = []
    for step in range(heads + 1, n):
        plan.append((0, step))
        plan.append((1, step - heads))
    for step in range(n - heads, n - 1):
        plan.append((1, step))
    per_step = -(-len(jobs) // (len(plan) - 1))
    for chunk, step in plan:
        for _ in range(min(per_step, len(jobs))):
            jobs.pop(0)()
        spread.step(chunk, step)
    for job in jobs:
        job()
    spread.step(1, n - 1)
    for chunk in range(samples):
        spread.settle(chunk, n - 1)

    half = shard // 2

    def rows_of(whose, origin, way):
        return pl.ds(pl.multiple_of(((whose * n + origin) * 2 + way) * half, half), half)

    share_out = Gather(
        ring,
        pairs,
        2,
        lambda way, chunk: mine.at[chunk, way],
        lambda way, chunk, whose, origin: weights[chunk].at[rows_of(whose, origin, way)],
        sems[8:],
    )
    for copy in swaps:
        copy.wait()
    for chunk in range(2):
        grad = mul(
            columns[...].reshape(pairs * samples * tokens, shard),
            every[chunk].reshape(pairs * samples * tokens, model_columns),
            ((0,), (0,)),
        ).astype(BF16)
        mine[chunk] = grad.reshape(mine.shape[1:])
        for way in range(2):
            share_out.start(way, chunk, 0)
    result = total[...]
    for at, copy in enumerate(copies):
        copy.wait()
        result = result + arrived[at].astype(F32)
    vision_out[...] = result.astype(BF16)
    for chunk in range(2):
        for way in range(2):
            weights[chunk][rows_of(lane, here, way), :] = mine[chunk, way]
    for step in range(1, n):
        for chunk in range(2):
            share_out.step(chunk, step)
    for chunk in range(2):
        share_out.settle(chunk, n - 1)

    for copy in pushes:
        copy.wait_send()
    for chunk in range(samples):
        for way in range(2):
            for step in range(n - 1):
                scatter_copy(way, chunk, step).wait_send()
    for each in (gather, spread, share_out):
        each.drain()


def emit_kernel(query_ref, vision_ref, key_ref, value_ref, query_out, vision_out, key_out, value_out, staged, sem, own_sem):
    heads, _, _, wide = query_ref.shape
    passed = [pltpu.make_async_copy(vision_ref, vision_out, own_sem.at[heads])]
    for at in range(heads):
        passed.append(
            pltpu.make_async_copy(
                query_ref.at[at], query_out.at[:, :, at * wide : (at + 1) * wide], own_sem.at[at]
            )
        )
    slots, block = staged.shape[:2]
    blocks = key_out.shape[0] // block
    copies = []
    for at in range(2 * blocks):
        kind, span = at // blocks, pl.ds(at % blocks * block, block)
        slot = at % slots
        if at >= slots:
            copies[at - slots].wait()
        staged[slot] = (key_ref, value_ref)[kind][span, :].astype(F32)
        copy = pltpu.make_async_copy(staged.at[slot], (key_out, value_out)[kind].at[span], sem.at[slot])
        copy.start()
        copies.append(copy)
        if at < len(passed):
            passed[at].start()
    for copy in copies[-slots:] + passed:
        copy.wait()


def emit(query_grad, vision_grad, key_grad, value_grad):
    rows, columns = key_grad.shape
    heads, samples, text_rows, wide = query_grad.shape
    grad = jax.ShapeDtypeStruct((rows, columns), F32)
    block = rows // 16
    dma = pltpu.SemaphoreType.DMA
    return pl.pallas_call(
        emit_kernel,
        out_shape=(
            jax.ShapeDtypeStruct((samples, text_rows, heads * wide), BF16),
            jax.ShapeDtypeStruct(vision_grad.shape, BF16),
            grad,
            grad,
        ),
        in_specs=[pl.BlockSpec(memory_space=VMEM)] * 4,
        out_specs=(pl.BlockSpec(memory_space=pltpu.HBM),) * 4,
        scratch_shapes=[VMEM((4, block, columns), F32), dma((4,)), dma((heads + 1,))],
        compiler_params=pltpu.CompilerParams(vmem_limit_bytes=16 * 1024 * 1024),
        cost_estimate=pl.CostEstimate(flops=2 * rows * columns, bytes_accessed=8 * rows * columns, transcendentals=0),
        name="emit",
    )(query_grad, vision_grad, key_grad, value_grad)


def ring_sems(n, pairs, chunks):
    dma = pltpu.SemaphoreType.DMA
    pair = dma((2, n, chunks, max(pairs - 1, 1)))
    return [dma((2, n, chunks)), dma((2, n, chunks)), pair, pair]


def in_hbm(array):
    return pltpu.with_memory_space_constraint(array, pltpu.HBM)


def local(sizes, queries, vision, key_weight, value_weight, query_gain, key_gain, out_grad, tile_count):
    pairs, n, heads_cut = sizes
    samples, rows, width = vision.shape
    columns = key_weight.shape[1]
    head_dim = key_gain.shape[0]
    heads = columns // head_dim
    group = queries.shape[2] // columns
    block = (heads, rows, head_dim)
    by_head = (heads, samples, queries.shape[1], group * head_dim)
    share = width // heads_cut
    shard = width // (pairs * n)
    groups = samples if heads_cut % samples == 0 else 1
    kept = 1 if groups > 1 else samples
    tile = 512 if share % 512 == 0 else share
    moved = VMEM((max(heads_cut - 1, 1), samples * rows, share), BF16)
    dma = pltpu.SemaphoreType.DMA
    hbm = pl.BlockSpec(memory_space=pltpu.HBM)
    vmem = pl.BlockSpec(memory_space=VMEM)
    sent = 6 * samples * (n - 1) * rows * columns * 2 + 2 * (n - 1) * shard * columns * 2
    whole = pl.pallas_call(
        functools.partial(whole_kernel, sizes, group, n * rows // MAX_TILES, tile),
        out_shape=(
            jax.ShapeDtypeStruct(by_head, BF16),
            jax.ShapeDtypeStruct((samples * rows, share), BF16),
            jax.ShapeDtypeStruct((width, columns), BF16),
            jax.ShapeDtypeStruct((width, columns), BF16),
        ),
        in_specs=[hbm] * 8,
        out_specs=(vmem,) * 4,
        scratch_shapes=[
            VMEM((1, samples), jnp.int32),
            VMEM((1, head_dim), F32),
            VMEM((1, head_dim), F32),
            VMEM(by_head, BF16),
            VMEM(by_head, BF16),
            VMEM(vision.shape, BF16),
            VMEM((2, samples, *block), BF16),
            VMEM((samples, *block), F32),
            VMEM((2, samples, n, *block), BF16),
            VMEM((2, samples, n, *block), BF16),
            VMEM((2, samples, n - 1, *block), BF16),
            VMEM((pairs, samples, n, rows, shard), BF16),
            VMEM((2, samples, rows, columns), BF16),
            moved,
            moved,
            VMEM((samples * rows, share), F32),
            VMEM((2, pairs, samples, n, rows, columns), BF16),
            VMEM((2, 2, shard // 2, columns), BF16),
            dma((4 + 2 * CUTS + 2 * heads,)),
            dma((kept,)),
            dma((kept, pairs * n)),
            dma((kept, pairs * n)),
            dma((pairs, max(groups - 1, 1))),
            dma((pairs, max(groups - 1, 1))),
            dma((2, n, samples)),
            dma((2, n, samples)),
            dma((max(heads_cut - 1, 1),)),
            dma((max(heads_cut - 1, 1),)),
        ]
        + ring_sems(n, 1, samples)
        + ring_sems(n, pairs, samples)
        + ring_sems(n, pairs, 2),
        compiler_params=pltpu.CompilerParams(
            collective_id=1, has_side_effects=True, vmem_limit_bytes=LIMIT
        ),
        cost_estimate=pl.CostEstimate(flops=25_000_000_000, bytes_accessed=sent, transcendentals=0),
        name="whole",
    )(
        *map(
            in_hbm,
            (
                tile_count[None],
                queries,
                vision,
                key_weight,
                value_weight,
                query_gain[None],
                key_gain[None],
                out_grad,
            ),
        )
    )
    query_grad, vision_grad, key_grad, value_grad = emit(*whole)
    return query_grad, vision_grad.reshape(samples, rows, share), key_grad, value_grad


LIMIT = 38 * 1024 * 1024


def solution(mesh):
    sizes = (mesh.shape["dp"], mesh.shape["seq"], mesh.shape["mp"])
    in_specs = (
        P("dp", "seq", "mp"),
        P("dp", "seq", None),
        P(None, "mp"),
        P(None, "mp"),
        P(),
        P(),
        P("dp", "seq", "mp"),
        P("dp"),
    )
    out_specs = (P("dp", "seq", "mp"), P("dp", "seq", "mp"), P(None, "mp"), P(None, "mp"))
    return jax.shard_map(
        functools.partial(local, sizes), mesh=mesh, in_specs=in_specs, out_specs=out_specs, check_vma=False
    )
```

```python
import functools

import jax
import jax.numpy as jnp
from jax import lax
from jax.experimental import pallas as pl
from jax.experimental.pallas import tpu as pltpu
from jax.sharding import PartitionSpec as P

MAX_TILES = 4
EPS = 1e-05
NEG = -1e30
CUTS = 4
EARLY_PUSHES = 7
MESH = pl.DeviceIdType.MESH
VMEM = pltpu.VMEM
F32 = jnp.float32
BF16 = jnp.bfloat16


def norm_back(raw, inverse, gain, upstream):
    weighted = upstream * gain
    return inverse * weighted - raw * inverse * inverse * inverse * jnp.mean(
        weighted * raw, axis=-1, keepdims=True
    )


def inverse_of(raw):
    return lax.rsqrt(jnp.mean(raw * raw, axis=-1, keepdims=True) + EPS)


def seq_of(place, n):
    half = place // (n // 2)
    along = place + half * (n - 1 - 2 * place)
    return 2 * along + half


def place_of(index, n):
    side = index % 2
    along = index // 2
    return along + side * (n - 1 - 2 * along)


def greet(devices):
    barrier = pltpu.get_barrier_semaphore()
    for device in devices:
        pl.semaphore_signal(barrier, inc=1, device_id=device, device_id_type=MESH)
    return lambda: pl.semaphore_wait(barrier, len(devices))


def mul(left, right, dims):
    return lax.dot_general(left, right, (dims, ((), ())), preferred_element_type=F32)


def remote(source, target, send_sem, recv_sem, device):
    return pltpu.make_async_remote_copy(
        src_ref=source,
        dst_ref=target,
        send_sem=send_sem,
        recv_sem=recv_sem,
        device_id=device,
        device_id_type=MESH,
    )


class Ring:
    def __init__(self, n):
        self.n = n
        self.here = lax.axis_index("seq")
        self.place = place_of(self.here, n)
        self.nexts = (seq_of((self.place + 1) % n, n), seq_of((self.place + n - 1) % n, n))

    def origin(self, way, step):
        n, place = self.n, self.place
        return seq_of((place + n - step) % n if way == 0 else (place + step) % n, n)

    def dest(self, way, away):
        n, place = self.n, self.place
        return seq_of((place + away) % n if way == 0 else (place + n - away) % n, n)

    def reach(self, way, kind):
        return self.n // 2 if way == kind else self.n - 1 - self.n // 2


def when(step, below, most=None):
    def run(body):
        known = step if isinstance(step, int) else most
        if known is not None and known < below:
            body()
        elif not isinstance(step, int):
            pl.when(step < below)(body)

    return run


def is_first(step):
    return isinstance(step, int) and step == 0


class Gather:
    def __init__(self, ring, pairs, chunks, cuts, source, target, sems):
        self.ring, self.pairs, self.chunks, self.cuts = ring, pairs, chunks, cuts
        self.source, self.target, self.sems = source, target, sems
        self.lane = lax.axis_index("dp")

    def block(self, way, kind, chunk, step, cut):
        target = self.target(kind, chunk, self.lane, self.ring.origin(way, step), cut)
        return self.source(kind, chunk, cut) if is_first(step) else target, target

    def ring_copy(self, way, kind, chunk, step, cut):
        at = (way, step, kind * self.chunks + chunk, cut)
        block = self.block(way, kind, chunk, step, cut)
        return remote(*block, self.sems[0].at[at], self.sems[1].at[at], {"seq": self.ring.nexts[way]})

    def pair_copy(self, way, kind, chunk, step, cut, turn):
        at = (way, step, kind * self.chunks + chunk, cut, turn)
        block = self.block(way, kind, chunk, step, cut)
        other = {"dp": (self.lane + 1 + turn) % self.pairs}
        return remote(*block, self.sems[2].at[at], self.sems[3].at[at], other)

    def send(self, way, kind, chunk, step, cut, most=None):
        @when(step, self.ring.reach(way, kind), most)
        def _():
            self.ring_copy(way, kind, chunk, step, cut).start()

        if not is_first(step) or way == kind:
            for turn in range(self.pairs - 1):
                self.pair_copy(way, kind, chunk, step, cut, turn).start()

    def start(self, chunk, kinds=(0, 1)):
        for cut in range(self.cuts):
            for kind in kinds:
                for way in range(2):
                    self.send(way, kind, chunk, 0, cut)

    def step(self, chunk, step, cuts=None, most=None):
        for cut in range(self.cuts) if cuts is None else cuts:
            for kind in range(2):
                for way in range(2):

                    @when(step, self.ring.reach(way, kind) + 1, most)
                    def _():
                        self.ring_copy(way, kind, chunk, step - 1, cut).wait_recv()
                        self.send(way, kind, chunk, step, cut, most)

    def parcels(self):
        for chunk in range(self.chunks):
            for kind in range(2):
                for way in range(2):
                    for cut in range(self.cuts):
                        yield way, kind, chunk, cut

    def pair_copies(self, only=None):
        for way, kind, chunk, cut in self.parcels():
            if only is not None and chunk != only:
                continue
            for step in range(0 if way == kind else 1, self.ring.reach(way, kind) + 1):
                for turn in range(self.pairs - 1):
                    yield self.pair_copy(way, kind, chunk, step, cut, turn)

    def settle(self, only=None):
        for copy in self.pair_copies(only):
            copy.wait_recv()

    def drain(self):
        for copy in self.pair_copies():
            copy.wait_send()
        for way, kind, chunk, cut in self.parcels():
            for step in range(self.ring.reach(way, kind)):
                self.ring_copy(way, kind, chunk, step, cut).wait_send()


def whole_kernel(sizes, group, tile_tokens, tile, tiles_hbm, query_hbm, vision_hbm, key_hbm, value_hbm, query_gain_hbm,
                 key_gain_hbm, grad_hbm, query_out, vision_out, key_weight, value_weight, tiles_ref, query_gain, key_gain, queries,
                 out_grad, vision, own, raw_keys,
                 gathered, parts, held, columns, grads, leaving, arrived, total, every, mine, partial, load_sem, own_sem,
                 push_send, push_recv, mate_send, mate_recv, scatter_send, scatter_recv, leave_sem, arrive_sem, *sems):
    pairs, n, heads_cut = sizes
    ring = Ring(n)
    weights = (key_weight, value_weight)
    here, lane, me = ring.here, lax.axis_index("dp"), lax.axis_index("mp")
    samples, rows, width = vision.shape
    heads, _, text_rows, wide = queries.shape
    head_dim = key_gain.shape[1]
    model_columns = heads * head_dim
    tokens = n * rows
    reach = n // 2
    scale = head_dim ** (-0.5)
    depth = width // CUTS
    shard = columns.shape[-1]
    groups = samples if heads_cut % samples == 0 else 1

    loads = [pltpu.make_async_copy(vision_hbm, vision, load_sem.at[0])]
    for at, source in enumerate((key_hbm, value_hbm)):
        for cut in range(CUTS):
            span = pl.ds(cut * depth, depth)
            loads.append(
                pltpu.make_async_copy(source.at[span], weights[at].at[span], load_sem.at[1 + at * CUTS + cut])
            )
    later = [(key_gain_hbm, key_gain), (query_gain_hbm, query_gain), (tiles_hbm, tiles_ref)]
    for head in range(heads):
        for source, target in ((query_hbm, queries), (grad_hbm, out_grad)):
            later.append((source.at[:, :, head * wide : (head + 1) * wide], target.at[head]))
    for at, (source, target) in enumerate(later):
        loads.append(pltpu.make_async_copy(source, target, load_sem.at[1 + 2 * CUTS + at]))
    for load in loads:
        load.start()

    peers = [((lane + shift // n) % pairs, (here + shift % n) % n) for shift in range(1, pairs * n)]
    mates = [(me + shift) % heads_cut for shift in range(1, heads_cut)]
    all_here = greet([{"dp": peer[0], "seq": peer[1]} for peer in peers] + [{"mp": mate} for mate in mates])
    loads[0].wait()

    seat = me % groups
    kept = [seat] if groups > 1 else list(range(samples))

    def columns_of(sample, pair, index, held_in=None):
        held_in = vision if held_in is None else held_in
        return held_in.at[sample, :, pl.ds(pl.multiple_of((pair * n + index) * shard, shard), shard)]

    def pushes(shift):
        peer = (lane + shift // n) % pairs, (here + shift % n) % n
        return [
            remote(
                columns_of(sample, *peer),
                columns.at[lane, sample, here],
                push_send.at[at, shift],
                push_recv.at[at, shift],
                {"dp": peer[0], "seq": peer[1]},
            )
            for at, sample in enumerate(kept)
        ]

    at_once = EARLY_PUSHES
    each_time = -(-(pairs * n - 1 - at_once) // (2 * heads))

    def push_some(turn):
        for at in range(each_time):
            shift = 1 + at_once + turn * each_time + at

            @pl.when(shift < pairs * n)
            def _():
                for copy in pushes(shift):
                    copy.start()

    mine_here = [
        pltpu.make_async_copy(
            columns_of(sample, lane, here, vision_hbm), columns.at[lane, sample, here], own_sem.at[at]
        )
        for at, sample in enumerate(kept)
    ]
    for copy in mine_here:
        copy.start()
    swaps = [
        remote(
            columns.at[pair, seat],
            columns.at[pair, seat],
            mate_send.at[pair, at],
            mate_recv.at[pair, at],
            {"mp": me - seat + (seat + 1 + at) % groups},
        )
        for pair in range(pairs)
        for at in range(groups - 1)
    ]

    gather = Gather(
        ring,
        1,
        samples,
        heads,
        lambda kind, chunk, cut: own.at[kind, chunk, cut],
        lambda kind, chunk, whose, origin, cut: gathered.at[kind, chunk, origin, cut],
        sems[:4],
    )

    def project(at):
        product = None
        for cut in range(CUTS):
            loads[1 + at * CUTS + cut].wait()
            left = vision[:, :, cut * depth : (cut + 1) * depth].reshape(samples * rows, depth)
            part = jnp.dot(left, weights[at][cut * depth : (cut + 1) * depth], preferred_element_type=F32)
            product = part if product is None else product + part
        return product

    product = project(0)
    loads[1 + 2 * CUTS].wait()
    for at in range(heads):
        span = slice(at * head_dim, (at + 1) * head_dim)
        head = product[:, span]
        normed = (head * inverse_of(head) * key_gain[...]).astype(BF16)
        raw_keys[:, at] = head.reshape(samples, rows, head_dim)
        own[0, :, at] = normed.reshape(samples, rows, head_dim)
    all_here()
    gather.start(0, (0,))
    for shift in range(1, 1 + at_once):
        for copy in pushes(shift):
            copy.start()
    product = project(1).astype(BF16)
    for at in range(heads):
        own[1, :, at] = product[:, at * head_dim : (at + 1) * head_dim].reshape(samples, rows, head_dim)
    gather.start(0, (1,))
    for at in range(2):
        gathered[at, :, here] = own[at]

    for step in range(1, reach + 1):
        gather.step(0, step)
        if step == max(reach - 1, 1):
            gather.start(1)

    def attend(sample, head, midway):
        live = tiles_ref[:, sample : sample + 1] * tile_tokens

        def stacked(ref):
            cuts = [ref[head, sample, :, at * head_dim : (at + 1) * head_dim] for at in range(group)]
            return jnp.concatenate(cuts, axis=0)

        raw = stacked(queries).astype(F32)
        outs = stacked(out_grad)
        gain = query_gain[...]
        inverse = inverse_of(raw)
        normed = (raw * inverse * gain).astype(BF16)
        keys = gathered[0, sample, :, head].reshape(tokens, head_dim)
        values = gathered[1, sample, :, head].reshape(tokens, head_dim)
        scores = mul(normed, keys, ((1,), (1,))) * scale
        token = lax.broadcasted_iota(jnp.int32, scores.shape, 1)
        scores = jnp.where(token < live, scores, NEG)
        expo = jnp.exp(scores - jnp.max(scores, axis=-1, keepdims=True))
        probs = expo * (1.0 / jnp.sum(expo, axis=-1, keepdims=True))
        probs_b = probs.astype(BF16)
        attn = mul(probs_b, values, ((1,), (0,))).astype(BF16)
        midway()
        delta = jnp.sum(outs.astype(F32) * attn.astype(F32), axis=-1, keepdims=True)
        dprobs = mul(outs, values, ((1,), (1,)))
        dscores = (probs * (dprobs - delta)).astype(BF16)
        value_part = mul(probs_b, outs, ((0,), (0,))).astype(BF16)
        key_part = (mul(dscores, normed, ((0,), (0,))) * scale).astype(BF16)
        parts[0, sample, :, head] = key_part.reshape(n, rows, head_dim)
        parts[1, sample, :, head] = value_part.reshape(n, rows, head_dim)
        dnormed = mul(dscores, keys, ((1,), (0,))) * scale
        back = norm_back(raw, inverse, gain, dnormed).astype(BF16)
        for at in range(group):
            cut = slice(at * head_dim, (at + 1) * head_dim)
            query_out[head, sample, :, cut] = back[at * text_rows : (at + 1) * text_rows]

    def scatter_copy(way, kind, chunk, step, cut, block=None):
        target = held.at[way, kind, chunk, step, cut]
        at = (way, step, kind * samples + chunk, cut)
        block = target if block is None else block
        return remote(block, target, scatter_send.at[at], scatter_recv.at[at], {"seq": ring.nexts[way]})

    def scatter_start(chunk):
        for cut in range(heads):
            for kind in range(2):
                for way in range(2):
                    dest = ring.dest(way, ring.reach(way, kind))
                    scatter_copy(way, kind, chunk, 0, cut, parts.at[kind, chunk, dest, cut]).start()

    def scatter_step(chunk, step, cuts=range(heads), most=None):
        for cut in cuts:
            for kind in range(2):
                for way in range(2):

                    @when(step, ring.reach(way, kind), most)
                    def _():
                        scatter_copy(way, kind, chunk, step - 1, cut).wait_recv()
                        block = held.at[way, kind, chunk, step - 1, cut]
                        dest = ring.dest(way, ring.reach(way, kind) - step)
                        summed = block[...].astype(F32) + parts[kind, chunk, dest, cut].astype(F32)
                        block[...] = summed.astype(BF16)
                        scatter_copy(way, kind, chunk, step, cut, block).start()

    def scatter_sum(kind, chunk, cut):
        total = parts[kind, chunk, here, cut].astype(F32)
        for way in range(2):
            last = ring.reach(way, kind) - 1
            scatter_copy(way, kind, chunk, last, cut).wait_recv()
            total = total + held[way, kind, chunk, last, cut].astype(F32)
        return total

    def scatter_last(chunk):
        gain = key_gain[...]
        for at in range(heads):
            cut = slice(at * head_dim, (at + 1) * head_dim)
            raw = raw_keys[chunk, at]
            summed = scatter_sum(0, chunk, at)
            grads[0, chunk, :, cut] = norm_back(raw, inverse_of(raw), gain, summed).astype(BF16)
            grads[1, chunk, :, cut] = scatter_sum(1, chunk, at).astype(BF16)

    for load in loads[2 + 2 * CUTS :]:
        load.wait()

    early, late = range(heads - heads // 2), range(heads - heads // 2, heads)

    def first_sample(head, carry):
        gather.step(1, head + 1, early, heads)
        push_some(head)
        attend(0, head, lambda: gather.step(1, head + 1, late, heads))
        return carry

    lax.fori_loop(0, heads, first_sample, 0)
    for step in range(heads + 1, reach + 1):
        gather.step(1, step)
    scatter_start(0)

    def second_sample(head, carry):
        scatter_step(0, head + 1, early, heads)
        push_some(heads + head)
        attend(1, head, lambda: scatter_step(0, head + 1, late, heads))
        return carry

    lax.fori_loop(0, heads, second_sample, 0)
    for step in range(heads + 1, reach):
        scatter_step(0, step)
    scatter_start(1)

    row_cuts = row_cuts_of(rows)

    def rows_at(cut):
        return pl.ds(*row_cuts[cut])

    spread = Gather(
        ring,
        pairs,
        samples,
        len(row_cuts),
        lambda kind, chunk, cut: grads.at[kind, chunk, rows_at(cut)],
        lambda kind, chunk, whose, origin, cut: every.at[kind, whose, chunk, origin, rows_at(cut)],
        sems[4:8],
    )
    scatter_last(0)
    spread.start(0)
    for step in range(1, reach + 1):
        if step < reach:
            scatter_step(1, step)
        else:
            scatter_last(1)
            spread.start(1)
        spread.step(0, step)
        if step == 1:
            for shift in range(1, pairs * n):
                for copy in pushes(shift):
                    copy.wait_recv()
            for copy in mine_here:
                copy.wait()
            for copy in swaps:
                copy.start()
    for kind in range(2):
        every[kind, lane, :, here] = grads[kind]
    for copy in swaps:
        copy.wait()
    spread.settle(0)

    def product(kind, sample):
        return mul(
            columns[:, sample].reshape(pairs * tokens, shard),
            every[kind, :, sample].reshape(pairs * tokens, model_columns),
            ((0,), (0,)),
        )

    share = total.shape[1]
    tiles = share // tile
    copies = []

    def vision_part(owner, at):
        span = pl.ds(pl.multiple_of(owner * share + at * tile, tile), tile)
        part = None
        for kind in range(2):
            left = grads[kind].reshape(samples * rows, model_columns)
            term = mul(left, weights[kind][span, :], ((1,), (1,)))
            part = term if part is None else part + term
        return part

    def leave(at):
        copy = remote(leaving.at[at], arrived.at[at], leave_sem.at[at], arrive_sem.at[at], {"mp": mates[at]})
        copy.start()
        copies.append(copy)

    jobs = []
    for turn, owner in enumerate(mates + [me]):
        for at in range(tiles):

            def job(turn=turn, owner=owner, at=at):
                span = slice(at * tile, (at + 1) * tile)
                part = vision_part(owner, at)
                if turn == len(mates):
                    total[:, span] = part
                    return
                leaving[turn, :, span] = part.astype(BF16)
                if at == tiles - 1:
                    leave(turn)

            jobs.append(job)

    for kind in range(2):

        def job(kind=kind):
            partial[kind] = product(kind, 0)

        jobs.append(job)
    for step in range(1, reach + 1):
        if step < reach:
            for _ in range(-(-len(jobs) // (reach - step))):
                jobs.pop(0)()
        spread.step(1, step)
    spread.settle(1)

    share_cuts = mine.shape[1]
    cut_rows = shard // share_cuts

    def rows_of(whose, origin, cut):
        return pl.ds(pl.multiple_of(((whose * n + origin) * share_cuts + cut) * cut_rows, cut_rows), cut_rows)

    share_out = Gather(
        ring,
        pairs,
        1,
        share_cuts,
        lambda kind, chunk, cut: mine.at[kind, cut],
        lambda kind, chunk, whose, origin, cut: weights[kind].at[rows_of(whose, origin, cut)],
        sems[8:],
    )
    for kind in range(2):
        grad = partial[kind]
        for sample in range(1, samples):
            grad = grad + product(kind, sample)
        mine[kind] = grad.astype(BF16).reshape(mine.shape[1:])
        share_out.start(0, (kind,))
    result = total[...]
    for at, copy in enumerate(copies):
        copy.wait()
        result = result + arrived[at].astype(F32)
    vision_out[...] = result.astype(BF16)
    for kind in range(2):
        for cut in range(share_cuts):
            weights[kind][rows_of(lane, here, cut), :] = mine[kind, cut]
    for step in range(1, reach + 1):
        share_out.step(0, step)
    share_out.settle()

    for shift in range(1, pairs * n):
        for copy in pushes(shift):
            copy.wait_send()
    for chunk in range(samples):
        for kind in range(2):
            for way in range(2):
                for step in range(ring.reach(way, kind)):
                    for cut in range(heads):
                        scatter_copy(way, kind, chunk, step, cut).wait_send()
    for each in (gather, spread, share_out):
        each.drain()


def emit_kernel(query_ref, vision_ref, key_ref, value_ref, query_out, vision_out, key_out, value_out, staged, sem, own_sem):
    heads, _, _, wide = query_ref.shape
    passed = [pltpu.make_async_copy(vision_ref, vision_out, own_sem.at[heads])]
    for at in range(heads):
        passed.append(
            pltpu.make_async_copy(
                query_ref.at[at], query_out.at[:, :, at * wide : (at + 1) * wide], own_sem.at[at]
            )
        )
    slots, block = staged.shape[:2]
    blocks = key_out.shape[0] // block
    copies = []
    for at in range(2 * blocks):
        kind, span = at // blocks, pl.ds(at % blocks * block, block)
        slot = at % slots
        if at >= slots:
            copies[at - slots].wait()
        staged[slot] = (key_ref, value_ref)[kind][span, :].astype(F32)
        copy = pltpu.make_async_copy(staged.at[slot], (key_out, value_out)[kind].at[span], sem.at[slot])
        copy.start()
        copies.append(copy)
        if at < len(passed):
            passed[at].start()
    for copy in copies[-slots:] + passed:
        copy.wait()


def emit(query_grad, vision_grad, key_grad, value_grad):
    rows, columns = key_grad.shape
    heads, samples, text_rows, wide = query_grad.shape
    grad = jax.ShapeDtypeStruct((rows, columns), F32)
    block = rows // 16
    dma = pltpu.SemaphoreType.DMA
    return pl.pallas_call(
        emit_kernel,
        out_shape=(
            jax.ShapeDtypeStruct((samples, text_rows, heads * wide), BF16),
            jax.ShapeDtypeStruct(vision_grad.shape, BF16),
            grad,
            grad,
        ),
        in_specs=[pl.BlockSpec(memory_space=VMEM)] * 4,
        out_specs=(pl.BlockSpec(memory_space=pltpu.HBM),) * 4,
        scratch_shapes=[VMEM((4, block, columns), F32), dma((4,)), dma((heads + 1,))],
        compiler_params=pltpu.CompilerParams(vmem_limit_bytes=16 * 1024 * 1024),
        cost_estimate=pl.CostEstimate(flops=2 * rows * columns, bytes_accessed=8 * rows * columns, transcendentals=0),
        name="emit",
    )(query_grad, vision_grad, key_grad, value_grad)


def row_cuts_of(rows):
    first = -(-rows // 32) * 16
    return [(0, first), (first, rows - first)] if rows % 16 == 0 and rows > 16 else [(0, rows)]


def ring_sems(n, pairs, chunks, cuts):
    dma = pltpu.SemaphoreType.DMA
    steps = n // 2
    pair = dma((2, steps + 1, 2 * chunks, cuts, max(pairs - 1, 1)))
    return [dma((2, steps, 2 * chunks, cuts)), dma((2, steps, 2 * chunks, cuts)), pair, pair]


def in_hbm(array):
    return pltpu.with_memory_space_constraint(array, pltpu.HBM)


def local(sizes, queries, vision, key_weight, value_weight, query_gain, key_gain, out_grad, tile_count):
    pairs, n, heads_cut = sizes
    samples, rows, width = vision.shape
    columns = key_weight.shape[1]
    head_dim = key_gain.shape[0]
    heads = columns // head_dim
    group = queries.shape[2] // columns
    block = (heads, rows, head_dim)
    by_head = (heads, samples, queries.shape[1], group * head_dim)
    share = width // heads_cut
    shard = width // (pairs * n)
    groups = samples if heads_cut % samples == 0 else 1
    kept = 1 if groups > 1 else samples
    tile = 512 if share % 512 == 0 else share
    share_cuts = 4 if shard % 64 == 0 else 1
    moved = VMEM((max(heads_cut - 1, 1), samples * rows, share), BF16)
    dma = pltpu.SemaphoreType.DMA
    hbm = pl.BlockSpec(memory_space=pltpu.HBM)
    vmem = pl.BlockSpec(memory_space=VMEM)
    sent = 6 * samples * (n - 1) * rows * columns * 2 + 2 * (n - 1) * shard * columns * 2
    whole = pl.pallas_call(
        functools.partial(whole_kernel, sizes, group, n * rows // MAX_TILES, tile),
        out_shape=(
            jax.ShapeDtypeStruct(by_head, BF16),
            jax.ShapeDtypeStruct((samples * rows, share), BF16),
            jax.ShapeDtypeStruct((width, columns), BF16),
            jax.ShapeDtypeStruct((width, columns), BF16),
        ),
        in_specs=[hbm] * 8,
        out_specs=(vmem,) * 4,
        scratch_shapes=[
            VMEM((1, samples), jnp.int32),
            VMEM((1, head_dim), F32),
            VMEM((1, head_dim), F32),
            VMEM(by_head, BF16),
            VMEM(by_head, BF16),
            VMEM(vision.shape, BF16),
            VMEM((2, samples, *block), BF16),
            VMEM((samples, *block), F32),
            VMEM((2, samples, n, *block), BF16),
            VMEM((2, samples, n, *block), BF16),
            VMEM((2, 2, samples, n // 2, *block), BF16),
            VMEM((pairs, samples, n, rows, shard), BF16),
            VMEM((2, samples, rows, columns), BF16),
            moved,
            moved,
            VMEM((samples * rows, share), F32),
            VMEM((2, pairs, samples, n, rows, columns), BF16),
            VMEM((2, share_cuts, shard // share_cuts, columns), BF16),
            VMEM((2, shard, columns), F32),
            dma((4 + 2 * CUTS + 2 * heads,)),
            dma((kept,)),
            dma((kept, pairs * n)),
            dma((kept, pairs * n)),
            dma((pairs, max(groups - 1, 1))),
            dma((pairs, max(groups - 1, 1))),
            dma((2, n // 2, 2 * samples, heads)),
            dma((2, n // 2, 2 * samples, heads)),
            dma((max(heads_cut - 1, 1),)),
            dma((max(heads_cut - 1, 1),)),
        ]
        + ring_sems(n, 1, samples, heads)
        + ring_sems(n, pairs, samples, len(row_cuts_of(rows)))
        + ring_sems(n, pairs, 1, share_cuts),
        compiler_params=pltpu.CompilerParams(
            collective_id=1, has_side_effects=True, vmem_limit_bytes=LIMIT
        ),
        cost_estimate=pl.CostEstimate(flops=25_000_000_000, bytes_accessed=sent, transcendentals=0),
        name="whole",
    )(
        *map(
            in_hbm,
            (
                tile_count[None],
                queries,
                vision,
                key_weight,
                value_weight,
                query_gain[None],
                key_gain[None],
                out_grad,
            ),
        )
    )
    query_grad, vision_grad, key_grad, value_grad = emit(*whole)
    return query_grad, vision_grad.reshape(samples, rows, share), key_grad, value_grad


LIMIT = 38 * 1024 * 1024


def solution(mesh):
    sizes = (mesh.shape["dp"], mesh.shape["seq"], mesh.shape["mp"])
    in_specs = (
        P("dp", "seq", "mp"),
        P("dp", "seq", None),
        P(None, "mp"),
        P(None, "mp"),
        P(),
        P(),
        P("dp", "seq", "mp"),
        P("dp"),
    )
    out_specs = (P("dp", "seq", "mp"), P("dp", "seq", "mp"), P(None, "mp"), P(None, "mp"))
    return jax.shard_map(
        functools.partial(local, sizes), mesh=mesh, in_specs=in_specs, out_specs=out_specs, check_vma=False
    )
```

```python
import functools

import jax
import jax.numpy as jnp
from jax import lax
from jax.experimental import pallas as pl
from jax.experimental.pallas import tpu as pltpu
from jax.sharding import PartitionSpec as P

MAX_TILES = 4
EPS = 1e-05
NEG = -1e30
CUTS = 4
EARLY_PUSHES = 7
MESH = pl.DeviceIdType.MESH
VMEM = pltpu.VMEM
F32 = jnp.float32
BF16 = jnp.bfloat16


def norm_back(raw, inverse, gain, upstream):
    weighted = upstream * gain
    return inverse * weighted - raw * inverse * inverse * inverse * jnp.mean(
        weighted * raw, axis=-1, keepdims=True
    )


def inverse_of(raw):
    return lax.rsqrt(jnp.mean(raw * raw, axis=-1, keepdims=True) + EPS)


def seq_of(place, n):
    half = place // (n // 2)
    along = place + half * (n - 1 - 2 * place)
    return 2 * along + half


def place_of(index, n):
    side = index % 2
    along = index // 2
    return along + side * (n - 1 - 2 * along)


def greet(devices):
    barrier = pltpu.get_barrier_semaphore()
    for device in devices:
        pl.semaphore_signal(barrier, inc=1, device_id=device, device_id_type=MESH)
    return lambda: pl.semaphore_wait(barrier, len(devices))


def mul(left, right, dims):
    return lax.dot_general(left, right, (dims, ((), ())), preferred_element_type=F32)


def remote(source, target, send_sem, recv_sem, device):
    return pltpu.make_async_remote_copy(
        src_ref=source,
        dst_ref=target,
        send_sem=send_sem,
        recv_sem=recv_sem,
        device_id=device,
        device_id_type=MESH,
    )


class Ring:
    def __init__(self, n):
        self.n = n
        self.here = lax.axis_index("seq")
        self.place = place_of(self.here, n)
        self.nexts = (seq_of((self.place + 1) % n, n), seq_of((self.place + n - 1) % n, n))
        self.away = {(way, step): self.at(way, step) for way in range(2) for step in range(n // 2 + 1)}

    def at(self, way, away):
        n, place = self.n, self.place
        return seq_of((place + n - away) % n if way == 0 else (place + away) % n, n)

    def origin(self, way, step):
        return self.away[way, step] if isinstance(step, int) else self.at(way, step)

    def dest(self, way, away):
        return self.origin(1 - way, away)

    def reach(self, way, kind):
        return self.n // 2 if way == kind else self.n - 1 - self.n // 2


def when(step, below, most=None):
    def run(body):
        known = step if isinstance(step, int) else most
        if known is not None and known < below:
            body()
        elif not isinstance(step, int):
            pl.when(step < below)(body)

    return run


def is_first(step):
    return isinstance(step, int) and step == 0


class Gather:
    def __init__(self, ring, pairs, chunks, cuts, source, target, some, sems):
        self.ring, self.pairs, self.chunks, self.cuts = ring, pairs, chunks, cuts
        self.source, self.target, self.some, self.sems = source, target, some, sems
        self.lane = lax.axis_index("dp")

    def block(self, way, kind, chunk, step, cut):
        target = self.target(kind, chunk, self.lane, self.ring.origin(way, step), cut)
        return self.source(kind, chunk, cut) if is_first(step) else target, target

    def ring_copy(self, way, kind, chunk, step, cut):
        at = (way, step, kind * self.chunks + chunk, cut)
        block = self.block(way, kind, chunk, step, cut)
        return remote(*block, self.sems[0].at[kind], self.sems[1].at[at], {"seq": self.ring.nexts[way]})

    def pair_copy(self, way, kind, chunk, step, cut, turn):
        block = self.block(way, kind, chunk, step, cut)
        other = {"dp": (self.lane + 1 + turn) % self.pairs}
        return remote(*block, self.sems[2].at[turn, kind], self.sems[3].at[turn, chunk, kind], other)

    def send(self, way, kind, chunk, step, cut, most=None):
        @when(step, self.ring.reach(way, kind), most)
        def _():
            self.ring_copy(way, kind, chunk, step, cut).start()

        if not is_first(step) or way == kind:
            for turn in range(self.pairs - 1):
                self.pair_copy(way, kind, chunk, step, cut, turn).start()

    def start(self, chunk, kinds=(0, 1)):
        for cut in range(self.cuts):
            for kind in kinds:
                for way in range(2):
                    self.send(way, kind, chunk, 0, cut)

    def step(self, chunk, step, cuts=None, most=None):
        for cut in range(self.cuts) if cuts is None else cuts:
            for kind in range(2):
                for way in range(2):

                    @when(step, self.ring.reach(way, kind) + 1, most)
                    def _():
                        self.ring_copy(way, kind, chunk, step - 1, cut).wait_recv()
                        self.send(way, kind, chunk, step, cut, most)

    def settle(self, chunk):
        near = {"seq": self.ring.nexts[0]}
        for turn in range(self.pairs - 1):
            for kind in range(2):
                ref = self.some(kind, 1, self.ring.n)
                sems = self.sems[2].at[turn, kind], self.sems[3].at[turn, chunk, kind]
                remote(ref, ref, *sems, near).wait_recv()

    def drain(self):
        near = {"seq": self.ring.nexts[0]}
        for kind in range(2):
            sends = [(self.sems[0].at[kind], self.ring.n - 1)]
            sends += [(self.sems[2].at[turn, kind], self.ring.n) for turn in range(self.pairs - 1)]
            for sem, count in sends:
                ref = self.some(kind, self.chunks, count)
                remote(ref, ref, sem, self.sems[1].at[0, 0, 0, 0], near).wait_send()


def whole_kernel(sizes, group, tile_tokens, tile, tiles_hbm, query_hbm, vision_hbm, key_hbm, value_hbm, query_gain_hbm,
                 key_gain_hbm, grad_hbm, query_out, vision_out, key_weight, value_weight, tiles_ref, query_gain, key_gain, queries,
                 out_grad, vision, own, raw_keys,
                 gathered, parts, held, columns, grads, leaving, arrived, total, every, mine, partial, load_sem, own_sem,
                 push_send, push_recv, mate_send, mate_recv, scatter_send, scatter_recv, leave_sem, arrive_sem, *sems):
    pairs, n, heads_cut = sizes
    ring = Ring(n)
    weights = (key_weight, value_weight)
    here, lane, me = ring.here, lax.axis_index("dp"), lax.axis_index("mp")
    samples, rows, width = vision.shape
    heads, _, text_rows, wide = queries.shape
    head_dim = key_gain.shape[1]
    model_columns = heads * head_dim
    tokens = n * rows
    reach = n // 2
    scale = head_dim ** (-0.5)
    depth = width // CUTS
    shard = columns.shape[-1]
    groups = samples if heads_cut % samples == 0 else 1

    loads = [pltpu.make_async_copy(vision_hbm, vision, load_sem.at[0])]
    for at, source in enumerate((key_hbm, value_hbm)):
        for cut in range(CUTS):
            span = pl.ds(cut * depth, depth)
            loads.append(
                pltpu.make_async_copy(source.at[span], weights[at].at[span], load_sem.at[1 + at * CUTS + cut])
            )
    later = [(key_gain_hbm, key_gain), (query_gain_hbm, query_gain), (tiles_hbm, tiles_ref)]
    for head in range(heads):
        for source, target in ((query_hbm, queries), (grad_hbm, out_grad)):
            later.append((source.at[:, :, head * wide : (head + 1) * wide], target.at[head]))
    for at, (source, target) in enumerate(later):
        loads.append(pltpu.make_async_copy(source, target, load_sem.at[1 + 2 * CUTS + at]))
    for load in loads:
        load.start()

    peers = [((lane + shift // n) % pairs, (here + shift % n) % n) for shift in range(1, pairs * n)]
    mates = [(me + shift) % heads_cut for shift in range(1, heads_cut)]
    all_here = greet([{"dp": peer[0], "seq": peer[1]} for peer in peers] + [{"mp": mate} for mate in mates])
    loads[0].wait()

    seat = me % groups
    kept = [seat] if groups > 1 else list(range(samples))

    def columns_of(sample, pair, index, held_in=None):
        held_in = vision if held_in is None else held_in
        return held_in.at[sample, :, pl.ds(pl.multiple_of((pair * n + index) * shard, shard), shard)]

    def pushes(shift):
        peer = (lane + shift // n) % pairs, (here + shift % n) % n
        return [
            remote(
                columns_of(sample, *peer),
                columns.at[lane, sample, here],
                push_send.at[at, shift],
                push_recv.at[at, shift],
                {"dp": peer[0], "seq": peer[1]},
            )
            for at, sample in enumerate(kept)
        ]

    at_once = EARLY_PUSHES
    each_time = -(-(pairs * n - 1 - at_once) // (2 * heads))

    def push_some(turn):
        for at in range(each_time):
            shift = 1 + at_once + turn * each_time + at

            @pl.when(shift < pairs * n)
            def _():
                for copy in pushes(shift):
                    copy.start()

    mine_here = [
        pltpu.make_async_copy(
            columns_of(sample, lane, here, vision_hbm), columns.at[lane, sample, here], own_sem.at[at]
        )
        for at, sample in enumerate(kept)
    ]
    for copy in mine_here:
        copy.start()
    swaps = [
        remote(
            columns.at[pair, seat],
            columns.at[pair, seat],
            mate_send.at[pair, at],
            mate_recv.at[pair, at],
            {"mp": me - seat + (seat + 1 + at) % groups},
        )
        for pair in range(pairs)
        for at in range(groups - 1)
    ]

    gather = Gather(
        ring,
        1,
        samples,
        heads,
        lambda kind, chunk, cut: own.at[kind, chunk, cut],
        lambda kind, chunk, whose, origin, cut: gathered.at[kind, chunk, origin, cut],
        lambda kind, chunks, count: gathered.at[kind, :chunks, :count],
        sems[:4],
    )

    def project(at):
        product = None
        for cut in range(CUTS):
            loads[1 + at * CUTS + cut].wait()
            left = vision[:, :, cut * depth : (cut + 1) * depth].reshape(samples * rows, depth)
            part = jnp.dot(left, weights[at][cut * depth : (cut + 1) * depth], preferred_element_type=F32)
            product = part if product is None else product + part
        return product

    product = project(0)
    loads[1 + 2 * CUTS].wait()
    for at in range(heads):
        span = slice(at * head_dim, (at + 1) * head_dim)
        head = product[:, span]
        normed = (head * inverse_of(head) * key_gain[...]).astype(BF16)
        raw_keys[:, at] = head.reshape(samples, rows, head_dim)
        own[0, :, at] = normed.reshape(samples, rows, head_dim)
    all_here()
    gather.start(0, (0,))
    for shift in range(1, 1 + at_once):
        for copy in pushes(shift):
            copy.start()
    product = project(1).astype(BF16)
    for at in range(heads):
        own[1, :, at] = product[:, at * head_dim : (at + 1) * head_dim].reshape(samples, rows, head_dim)
    gather.start(0, (1,))
    for at in range(2):
        gathered[at, :, here] = own[at]

    for step in range(1, reach + 1):
        gather.step(0, step)
        if step == max(reach - 1, 1):
            gather.start(1)

    def attend(sample, head, midway):
        live = tiles_ref[:, sample : sample + 1] * tile_tokens

        def stacked(ref):
            cuts = [ref[head, sample, :, at * head_dim : (at + 1) * head_dim] for at in range(group)]
            return jnp.concatenate(cuts, axis=0)

        raw = stacked(queries).astype(F32)
        outs = stacked(out_grad)
        gain = query_gain[...]
        inverse = inverse_of(raw)
        normed = (raw * inverse * gain).astype(BF16)
        keys = gathered[0, sample, :, head].reshape(tokens, head_dim)
        values = gathered[1, sample, :, head].reshape(tokens, head_dim)
        scores = mul(normed, keys, ((1,), (1,))) * scale
        token = lax.broadcasted_iota(jnp.int32, scores.shape, 1)
        scores = jnp.where(token < live, scores, NEG)
        expo = jnp.exp(scores - jnp.max(scores, axis=-1, keepdims=True))
        probs = expo * (1.0 / jnp.sum(expo, axis=-1, keepdims=True))
        probs_b = probs.astype(BF16)
        attn = mul(probs_b, values, ((1,), (0,))).astype(BF16)
        midway()
        delta = jnp.sum(outs.astype(F32) * attn.astype(F32), axis=-1, keepdims=True)
        dprobs = mul(outs, values, ((1,), (1,)))
        dscores = (probs * (dprobs - delta)).astype(BF16)
        value_part = mul(probs_b, outs, ((0,), (0,))).astype(BF16)
        key_part = (mul(dscores, normed, ((0,), (0,))) * scale).astype(BF16)
        parts[0, sample, :, head] = key_part.reshape(n, rows, head_dim)
        parts[1, sample, :, head] = value_part.reshape(n, rows, head_dim)
        dnormed = mul(dscores, keys, ((1,), (0,))) * scale
        back = norm_back(raw, inverse, gain, dnormed).astype(BF16)
        for at in range(group):
            cut = slice(at * head_dim, (at + 1) * head_dim)
            query_out[head, sample, :, cut] = back[at * text_rows : (at + 1) * text_rows]

    def scatter_copy(way, kind, chunk, step, cut, block=None):
        target = held.at[way, kind, chunk, step, cut]
        at = (way, step, kind * samples + chunk, cut)
        block = target if block is None else block
        return remote(block, target, scatter_send.at[0], scatter_recv.at[at], {"seq": ring.nexts[way]})

    def scatter_start(chunk):
        for cut in range(heads):
            for kind in range(2):
                for way in range(2):
                    dest = ring.dest(way, ring.reach(way, kind))
                    scatter_copy(way, kind, chunk, 0, cut, parts.at[kind, chunk, dest, cut]).start()

    def scatter_step(chunk, step, cuts=range(heads), most=None):
        for cut in cuts:
            for kind in range(2):
                for way in range(2):

                    @when(step, ring.reach(way, kind), most)
                    def _():
                        scatter_copy(way, kind, chunk, step - 1, cut).wait_recv()
                        block = held.at[way, kind, chunk, step - 1, cut]
                        dest = ring.dest(way, ring.reach(way, kind) - step)
                        summed = block[...].astype(F32) + parts[kind, chunk, dest, cut].astype(F32)
                        block[...] = summed.astype(BF16)
                        scatter_copy(way, kind, chunk, step, cut, block).start()

    def scatter_sum(kind, chunk, cut):
        total = parts[kind, chunk, here, cut].astype(F32)
        for way in range(2):
            last = ring.reach(way, kind) - 1
            scatter_copy(way, kind, chunk, last, cut).wait_recv()
            total = total + held[way, kind, chunk, last, cut].astype(F32)
        return total

    def scatter_last(chunk):
        gain = key_gain[...]
        for at in range(heads):
            cut = slice(at * head_dim, (at + 1) * head_dim)
            raw = raw_keys[chunk, at]
            summed = scatter_sum(0, chunk, at)
            grads[0, chunk, :, cut] = norm_back(raw, inverse_of(raw), gain, summed).astype(BF16)
            grads[1, chunk, :, cut] = scatter_sum(1, chunk, at).astype(BF16)

    for load in loads[2 + 2 * CUTS :]:
        load.wait()

    early, late = range(heads - heads // 2), range(heads - heads // 2, heads)

    def first_sample(head, carry):
        gather.step(1, head + 1, early, heads)
        push_some(head)
        attend(0, head, lambda: gather.step(1, head + 1, late, heads))
        return carry

    lax.fori_loop(0, heads, first_sample, 0)
    for step in range(heads + 1, reach + 1):
        gather.step(1, step)
    scatter_start(0)

    def second_sample(head, carry):
        scatter_step(0, head + 1, early, heads)
        push_some(heads + head)
        attend(1, head, lambda: scatter_step(0, head + 1, late, heads))
        return carry

    lax.fori_loop(0, heads, second_sample, 0)
    for step in range(heads + 1, reach):
        scatter_step(0, step)
    scatter_start(1)

    row_cuts = row_cuts_of(rows)

    def rows_at(cut):
        return pl.ds(*row_cuts[cut])

    spread = Gather(
        ring,
        pairs,
        samples,
        len(row_cuts),
        lambda kind, chunk, cut: grads.at[kind, chunk, rows_at(cut)],
        lambda kind, chunk, whose, origin, cut: every.at[kind, whose, chunk, origin, rows_at(cut)],
        lambda kind, chunks, count: every.at[kind, 0, :chunks, :count],
        sems[4:8],
    )
    scatter_last(0)
    spread.start(0)
    for step in range(1, reach + 1):
        if step < reach:
            scatter_step(1, step)
        else:
            scatter_last(1)
            spread.start(1)
        spread.step(0, step)
        if step == 1:
            for shift in range(1, pairs * n):
                for copy in pushes(shift):
                    copy.wait_recv()
            for copy in mine_here:
                copy.wait()
            for copy in swaps:
                copy.start()
    for kind in range(2):
        every[kind, lane, :, here] = grads[kind]
    for copy in swaps:
        copy.wait()
    spread.settle(0)

    def product(kind, sample):
        return mul(
            columns[:, sample].reshape(pairs * tokens, shard),
            every[kind, :, sample].reshape(pairs * tokens, model_columns),
            ((0,), (0,)),
        )

    share = total.shape[1]
    tiles = share // tile
    copies = []

    def vision_part(owner, at):
        span = pl.ds(pl.multiple_of(owner * share + at * tile, tile), tile)
        part = None
        for kind in range(2):
            left = grads[kind].reshape(samples * rows, model_columns)
            term = mul(left, weights[kind][span, :], ((1,), (1,)))
            part = term if part is None else part + term
        return part

    def leave(at):
        copy = remote(leaving.at[at], arrived.at[at], leave_sem.at[at], arrive_sem.at[at], {"mp": mates[at]})
        copy.start()
        copies.append(copy)

    jobs = []
    for turn, owner in enumerate(mates + [me]):
        for at in range(tiles):

            def job(turn=turn, owner=owner, at=at):
                span = slice(at * tile, (at + 1) * tile)
                part = vision_part(owner, at)
                if turn == len(mates):
                    total[:, span] = part
                    return
                leaving[turn, :, span] = part.astype(BF16)
                if at == tiles - 1:
                    leave(turn)

            jobs.append(job)

    for kind in range(2):

        def job(kind=kind):
            partial[kind] = product(kind, 0)

        jobs.append(job)
    for step in range(1, reach + 1):
        if step < reach:
            for _ in range(-(-len(jobs) // (reach - step))):
                jobs.pop(0)()
        spread.step(1, step)
    spread.settle(1)

    share_cuts = mine.shape[1]
    cut_rows = shard // share_cuts

    def rows_of(whose, origin, cut):
        return pl.ds(pl.multiple_of(((whose * n + origin) * share_cuts + cut) * cut_rows, cut_rows), cut_rows)

    share_out = Gather(
        ring,
        pairs,
        1,
        share_cuts,
        lambda kind, chunk, cut: mine.at[kind, cut],
        lambda kind, chunk, whose, origin, cut: weights[kind].at[rows_of(whose, origin, cut)],
        lambda kind, chunks, count: weights[kind].at[: count * shard],
        sems[8:],
    )
    for kind in range(2):
        grad = partial[kind]
        for sample in range(1, samples):
            grad = grad + product(kind, sample)
        mine[kind] = grad.astype(BF16).reshape(mine.shape[1:])
        share_out.start(0, (kind,))
    result = total[...]
    for at, copy in enumerate(copies):
        copy.wait()
        result = result + arrived[at].astype(F32)
    vision_out[...] = result.astype(BF16)
    for kind in range(2):
        for cut in range(share_cuts):
            weights[kind][rows_of(lane, here, cut), :] = mine[kind, cut]
    for step in range(1, reach + 1):
        share_out.step(0, step)
    share_out.settle(0)

    for shift in range(1, pairs * n):
        for copy in pushes(shift):
            copy.wait_send()
    sent = parts.at[:, :, : n - 1]
    remote(sent, sent, scatter_send.at[0], scatter_recv.at[0, 0, 0, 0], {"seq": ring.nexts[0]}).wait_send()
    for each in (gather, spread, share_out):
        each.drain()


def emit_kernel(query_ref, vision_ref, key_ref, value_ref, query_out, vision_out, key_out, value_out, staged, sem, own_sem):
    heads, _, _, wide = query_ref.shape
    passed = [pltpu.make_async_copy(vision_ref, vision_out, own_sem.at[heads])]
    for at in range(heads):
        passed.append(
            pltpu.make_async_copy(
                query_ref.at[at], query_out.at[:, :, at * wide : (at + 1) * wide], own_sem.at[at]
            )
        )
    slots, block = staged.shape[:2]
    blocks = key_out.shape[0] // block
    copies = []
    for at in range(2 * blocks):
        kind, span = at // blocks, pl.ds(at % blocks * block, block)
        slot = at % slots
        if at >= slots:
            copies[at - slots].wait()
        staged[slot] = (key_ref, value_ref)[kind][span, :].astype(F32)
        copy = pltpu.make_async_copy(staged.at[slot], (key_out, value_out)[kind].at[span], sem.at[slot])
        copy.start()
        copies.append(copy)
        if at < len(passed):
            passed[at].start()
    for copy in copies[-slots:] + passed:
        copy.wait()


def emit(query_grad, vision_grad, key_grad, value_grad):
    rows, columns = key_grad.shape
    heads, samples, text_rows, wide = query_grad.shape
    grad = jax.ShapeDtypeStruct((rows, columns), F32)
    block = rows // 16
    dma = pltpu.SemaphoreType.DMA
    return pl.pallas_call(
        emit_kernel,
        out_shape=(
            jax.ShapeDtypeStruct((samples, text_rows, heads * wide), BF16),
            jax.ShapeDtypeStruct(vision_grad.shape, BF16),
            grad,
            grad,
        ),
        in_specs=[pl.BlockSpec(memory_space=VMEM)] * 4,
        out_specs=(pl.BlockSpec(memory_space=pltpu.HBM),) * 4,
        scratch_shapes=[VMEM((4, block, columns), F32), dma((4,)), dma((heads + 1,))],
        compiler_params=pltpu.CompilerParams(vmem_limit_bytes=16 * 1024 * 1024),
        cost_estimate=pl.CostEstimate(flops=2 * rows * columns, bytes_accessed=8 * rows * columns, transcendentals=0),
        name="emit",
    )(query_grad, vision_grad, key_grad, value_grad)


def row_cuts_of(rows):
    first = -(-rows // 32) * 16
    return [(0, first), (first, rows - first)] if rows % 16 == 0 and rows > 16 else [(0, rows)]


def ring_sems(n, pairs, chunks, cuts):
    dma = pltpu.SemaphoreType.DMA
    others = max(pairs - 1, 1)
    return [dma((2,)), dma((2, n // 2, 2 * chunks, cuts)), dma((others, 2)), dma((others, chunks, 2))]


def in_hbm(array):
    return pltpu.with_memory_space_constraint(array, pltpu.HBM)


def local(sizes, queries, vision, key_weight, value_weight, query_gain, key_gain, out_grad, tile_count):
    pairs, n, heads_cut = sizes
    samples, rows, width = vision.shape
    columns = key_weight.shape[1]
    head_dim = key_gain.shape[0]
    heads = columns // head_dim
    group = queries.shape[2] // columns
    block = (heads, rows, head_dim)
    by_head = (heads, samples, queries.shape[1], group * head_dim)
    share = width // heads_cut
    shard = width // (pairs * n)
    groups = samples if heads_cut % samples == 0 else 1
    kept = 1 if groups > 1 else samples
    tile = 512 if share % 512 == 0 else share
    share_cuts = 4 if shard % 64 == 0 else 1
    moved = VMEM((max(heads_cut - 1, 1), samples * rows, share), BF16)
    dma = pltpu.SemaphoreType.DMA
    hbm = pl.BlockSpec(memory_space=pltpu.HBM)
    vmem = pl.BlockSpec(memory_space=VMEM)
    sent = 6 * samples * (n - 1) * rows * columns * 2 + 2 * (n - 1) * shard * columns * 2
    whole = pl.pallas_call(
        functools.partial(whole_kernel, sizes, group, n * rows // MAX_TILES, tile),
        out_shape=(
            jax.ShapeDtypeStruct(by_head, BF16),
            jax.ShapeDtypeStruct((samples * rows, share), BF16),
            jax.ShapeDtypeStruct((width, columns), BF16),
            jax.ShapeDtypeStruct((width, columns), BF16),
        ),
        in_specs=[hbm] * 8,
        out_specs=(vmem,) * 4,
        scratch_shapes=[
            VMEM((1, samples), jnp.int32),
            VMEM((1, head_dim), F32),
            VMEM((1, head_dim), F32),
            VMEM(by_head, BF16),
            VMEM(by_head, BF16),
            VMEM(vision.shape, BF16),
            VMEM((2, samples, *block), BF16),
            VMEM((samples, *block), F32),
            VMEM((2, samples, n, *block), BF16),
            VMEM((2, samples, n, *block), BF16),
            VMEM((2, 2, samples, n // 2, *block), BF16),
            VMEM((pairs, samples, n, rows, shard), BF16),
            VMEM((2, samples, rows, columns), BF16),
            moved,
            moved,
            VMEM((samples * rows, share), F32),
            VMEM((2, pairs, samples, n, rows, columns), BF16),
            VMEM((2, share_cuts, shard // share_cuts, columns), BF16),
            VMEM((2, shard, columns), F32),
            dma((4 + 2 * CUTS + 2 * heads,)),
            dma((kept,)),
            dma((kept, pairs * n)),
            dma((kept, pairs * n)),
            dma((pairs, max(groups - 1, 1))),
            dma((pairs, max(groups - 1, 1))),
            dma((1,)),
            dma((2, n // 2, 2 * samples, heads)),
            dma((max(heads_cut - 1, 1),)),
            dma((max(heads_cut - 1, 1),)),
        ]
        + ring_sems(n, 1, samples, heads)
        + ring_sems(n, pairs, samples, len(row_cuts_of(rows)))
        + ring_sems(n, pairs, 1, share_cuts),
        compiler_params=pltpu.CompilerParams(
            collective_id=1, has_side_effects=True, vmem_limit_bytes=LIMIT
        ),
        cost_estimate=pl.CostEstimate(flops=25_000_000_000, bytes_accessed=sent, transcendentals=0),
        name="whole",
    )(
        *map(
            in_hbm,
            (
                tile_count[None],
                queries,
                vision,
                key_weight,
                value_weight,
                query_gain[None],
                key_gain[None],
                out_grad,
            ),
        )
    )
    query_grad, vision_grad, key_grad, value_grad = emit(*whole)
    return query_grad, vision_grad.reshape(samples, rows, share), key_grad, value_grad


LIMIT = 38 * 1024 * 1024


def solution(mesh):
    sizes = (mesh.shape["dp"], mesh.shape["seq"], mesh.shape["mp"])
    in_specs = (
        P("dp", "seq", "mp"),
        P("dp", "seq", None),
        P(None, "mp"),
        P(None, "mp"),
        P(),
        P(),
        P("dp", "seq", "mp"),
        P("dp"),
    )
    out_specs = (P("dp", "seq", "mp"), P("dp", "seq", "mp"), P(None, "mp"), P(None, "mp"))
    return jax.shard_map(
        functools.partial(local, sizes), mesh=mesh, in_specs=in_specs, out_specs=out_specs, check_vma=False
    )
```

```python
import functools

import jax
import jax.numpy as jnp
from jax import lax
from jax.experimental import pallas as pl
from jax.experimental.pallas import tpu as pltpu
from jax.sharding import PartitionSpec as P

MAX_TILES = 4
EPS = 1e-05
NEG = -1e30
CUTS = 4
EARLY_PUSHES = 7
MESH = pl.DeviceIdType.MESH
VMEM = pltpu.VMEM
F32 = jnp.float32
BF16 = jnp.bfloat16


def norm_back(raw, inverse, gain, upstream):
    weighted = upstream * gain
    return inverse * weighted - raw * inverse * inverse * inverse * jnp.mean(
        weighted * raw, axis=-1, keepdims=True
    )


def inverse_of(raw):
    return lax.rsqrt(jnp.mean(raw * raw, axis=-1, keepdims=True) + EPS)


def seq_of(place, n):
    half = place // (n // 2)
    along = place + half * (n - 1 - 2 * place)
    return 2 * along + half


def place_of(index, n):
    side = index % 2
    along = index // 2
    return along + side * (n - 1 - 2 * along)


def greet(devices):
    barrier = pltpu.get_barrier_semaphore()
    for device in devices:
        pl.semaphore_signal(barrier, inc=1, device_id=device, device_id_type=MESH)
    return lambda: pl.semaphore_wait(barrier, len(devices))


def mul(left, right, dims):
    return lax.dot_general(left, right, (dims, ((), ())), preferred_element_type=F32)


def remote(source, target, send_sem, recv_sem, device):
    return pltpu.make_async_remote_copy(
        src_ref=source,
        dst_ref=target,
        send_sem=send_sem,
        recv_sem=recv_sem,
        device_id=device,
        device_id_type=MESH,
    )


class Ring:
    def __init__(self, n):
        self.n = n
        self.here = lax.axis_index("seq")
        self.place = place_of(self.here, n)
        self.nexts = (seq_of((self.place + 1) % n, n), seq_of((self.place + n - 1) % n, n))
        self.away = {(way, step): self.at(way, step) for way in range(2) for step in range(n // 2 + 1)}

    def at(self, way, away):
        n, place = self.n, self.place
        return seq_of((place + n - away) % n if way == 0 else (place + away) % n, n)

    def origin(self, way, step):
        return self.away[way, step] if isinstance(step, int) else self.at(way, step)

    def dest(self, way, away):
        return self.origin(1 - way, away)

    def reach(self, way, kind):
        return self.n // 2 if way == kind else self.n - 1 - self.n // 2


def when(step, below, most=None):
    def run(body):
        known = step if isinstance(step, int) else most
        if known is not None and known < below:
            body()
        elif not isinstance(step, int):
            pl.when(step < below)(body)

    return run


def is_first(step):
    return isinstance(step, int) and step == 0


class Gather:
    def __init__(self, ring, pairs, chunks, cuts, source, target, some, sems):
        self.ring, self.pairs, self.chunks, self.cuts = ring, pairs, chunks, cuts
        self.source, self.target, self.some, self.sems = source, target, some, sems
        self.lane = lax.axis_index("dp")

    def block(self, way, kind, chunk, step, cut):
        target = self.target(kind, chunk, self.lane, self.ring.origin(way, step), cut)
        return self.source(kind, chunk, cut) if is_first(step) else target, target

    def ring_copy(self, way, kind, chunk, step, cut):
        at = (way, step, kind * self.chunks + chunk, cut)
        block = self.block(way, kind, chunk, step, cut)
        return remote(*block, self.sems[0].at[kind], self.sems[1].at[at], {"seq": self.ring.nexts[way]})

    def pair_copy(self, way, kind, chunk, step, cut, turn):
        block = self.block(way, kind, chunk, step, cut)
        other = {"dp": (self.lane + 1 + turn) % self.pairs}
        return remote(*block, self.sems[2].at[turn, kind], self.sems[3].at[turn, chunk, kind], other)

    def send(self, way, kind, chunk, step, cut, most=None):
        @when(step, self.ring.reach(way, kind), most)
        def _():
            self.ring_copy(way, kind, chunk, step, cut).start()

        if not is_first(step) or way == kind:
            for turn in range(self.pairs - 1):
                self.pair_copy(way, kind, chunk, step, cut, turn).start()

    def start(self, chunk, kinds=(0, 1)):
        for cut in range(self.cuts):
            for kind in kinds:
                for way in range(2):
                    self.send(way, kind, chunk, 0, cut)

    def step(self, chunk, step, cuts=None, most=None):
        for cut in range(self.cuts) if cuts is None else cuts:
            for kind in range(2):
                for way in range(2):

                    @when(step, self.ring.reach(way, kind) + 1, most)
                    def _():
                        self.ring_copy(way, kind, chunk, step - 1, cut).wait_recv()
                        self.send(way, kind, chunk, step, cut, most)

    def settle(self, chunk):
        near = {"seq": self.ring.nexts[0]}
        for turn in range(self.pairs - 1):
            for kind in range(2):
                ref = self.some(kind, 1, self.ring.n)
                sems = self.sems[2].at[turn, kind], self.sems[3].at[turn, chunk, kind]
                remote(ref, ref, *sems, near).wait_recv()

    def drain(self):
        near = {"seq": self.ring.nexts[0]}
        for kind in range(2):
            sends = [(self.sems[0].at[kind], self.ring.n - 1)]
            sends += [(self.sems[2].at[turn, kind], self.ring.n) for turn in range(self.pairs - 1)]
            for sem, count in sends:
                ref = self.some(kind, self.chunks, count)
                remote(ref, ref, sem, self.sems[1].at[0, 0, 0, 0], near).wait_send()


def whole_kernel(sizes, group, tile_tokens, tile, tiles_hbm, query_hbm, vision_hbm, key_hbm, value_hbm, query_gain_hbm,
                 key_gain_hbm, grad_hbm, query_out, vision_out, key_weight, value_weight, tiles_ref, query_gain, key_gain, queries,
                 out_grad, vision, own, raw_keys,
                 gathered, parts, held, columns, grads, leaving, arrived, total, every, mine, partial, load_sem, own_sem,
                 push_send, push_recv, mate_send, mate_recv, scatter_send, scatter_recv, leave_sem, arrive_sem, *sems):
    pairs, n, heads_cut = sizes
    ring = Ring(n)
    weights = (key_weight, value_weight)
    here, lane, me = ring.here, lax.axis_index("dp"), lax.axis_index("mp")
    samples, rows, width = vision.shape
    heads, _, text_rows, wide = queries.shape
    head_dim = key_gain.shape[1]
    model_columns = heads * head_dim
    tokens = n * rows
    reach = n // 2
    scale = head_dim ** (-0.5)
    depth = width // CUTS
    shard = columns.shape[-1]
    groups = samples if heads_cut % samples == 0 else 1

    loads = [pltpu.make_async_copy(vision_hbm, vision, load_sem.at[0])]
    for at, source in enumerate((key_hbm, value_hbm)):
        for cut in range(CUTS):
            span = pl.ds(cut * depth, depth)
            loads.append(
                pltpu.make_async_copy(source.at[span], weights[at].at[span], load_sem.at[1 + at * CUTS + cut])
            )
    later = [(key_gain_hbm, key_gain), (query_gain_hbm, query_gain), (tiles_hbm, tiles_ref)]
    for head in range(heads):
        for source, target in ((query_hbm, queries), (grad_hbm, out_grad)):
            later.append((source.at[:, :, head * wide : (head + 1) * wide], target.at[head]))
    for at, (source, target) in enumerate(later):
        loads.append(pltpu.make_async_copy(source, target, load_sem.at[1 + 2 * CUTS + at]))
    small = loads[1 + 2 * CUTS : 4 + 2 * CUTS]
    for load in small + loads[: 1 + 2 * CUTS] + loads[4 + 2 * CUTS :]:
        load.start()

    peers = [((lane + shift // n) % pairs, (here + shift % n) % n) for shift in range(1, pairs * n)]
    mates = [(me + shift) % heads_cut for shift in range(1, heads_cut)]
    all_here = greet([{"dp": peer[0], "seq": peer[1]} for peer in peers] + [{"mp": mate} for mate in mates])
    loads[0].wait()

    seat = me % groups
    kept = [seat] if groups > 1 else list(range(samples))

    def columns_of(sample, pair, index, held_in=None):
        held_in = vision if held_in is None else held_in
        return held_in.at[sample, :, pl.ds(pl.multiple_of((pair * n + index) * shard, shard), shard)]

    def pushes(shift):
        peer = (lane + shift // n) % pairs, (here + shift % n) % n
        return [
            remote(
                columns_of(sample, *peer),
                columns.at[lane, sample, here],
                push_send.at[at, shift],
                push_recv.at[at, shift],
                {"dp": peer[0], "seq": peer[1]},
            )
            for at, sample in enumerate(kept)
        ]

    at_once = EARLY_PUSHES
    each_time = -(-(pairs * n - 1 - at_once) // (2 * heads))

    def push_some(turn):
        for at in range(each_time):
            shift = 1 + at_once + turn * each_time + at

            @pl.when(shift < pairs * n)
            def _():
                for copy in pushes(shift):
                    copy.start()

    mine_here = [
        pltpu.make_async_copy(
            columns_of(sample, lane, here, vision_hbm), columns.at[lane, sample, here], own_sem.at[at]
        )
        for at, sample in enumerate(kept)
    ]
    for copy in mine_here:
        copy.start()
    swaps = [
        remote(
            columns.at[pair, seat],
            columns.at[pair, seat],
            mate_send.at[pair, at],
            mate_recv.at[pair, at],
            {"mp": me - seat + (seat + 1 + at) % groups},
        )
        for pair in range(pairs)
        for at in range(groups - 1)
    ]

    gather = Gather(
        ring,
        1,
        samples,
        heads,
        lambda kind, chunk, cut: own.at[kind, chunk, cut],
        lambda kind, chunk, whose, origin, cut: gathered.at[kind, chunk, origin, cut],
        lambda kind, chunks, count: gathered.at[kind, :chunks, :count],
        sems[:4],
    )

    def project(at):
        product = None
        for cut in range(CUTS):
            loads[1 + at * CUTS + cut].wait()
            left = vision[:, :, cut * depth : (cut + 1) * depth].reshape(samples * rows, depth)
            part = jnp.dot(left, weights[at][cut * depth : (cut + 1) * depth], preferred_element_type=F32)
            product = part if product is None else product + part
        return product

    product = project(0)
    loads[1 + 2 * CUTS].wait()
    for at in range(heads):
        span = slice(at * head_dim, (at + 1) * head_dim)
        head = product[:, span]
        normed = (head * inverse_of(head) * key_gain[...]).astype(BF16)
        raw_keys[:, at] = head.reshape(samples, rows, head_dim)
        own[0, :, at] = normed.reshape(samples, rows, head_dim)
    all_here()
    gather.start(0, (0,))
    for shift in range(1, 1 + at_once):
        for copy in pushes(shift):
            copy.start()
    product = project(1).astype(BF16)
    for at in range(heads):
        own[1, :, at] = product[:, at * head_dim : (at + 1) * head_dim].reshape(samples, rows, head_dim)
    gather.start(0, (1,))
    for at in range(2):
        gathered[at, :, here] = own[at]

    for step in range(1, reach + 1):
        gather.step(0, step)
        if step == max(reach - 1, 1):
            gather.start(1)

    def attend(sample, head, midway):
        live = tiles_ref[:, sample : sample + 1] * tile_tokens

        def stacked(ref):
            cuts = [ref[head, sample, :, at * head_dim : (at + 1) * head_dim] for at in range(group)]
            return jnp.concatenate(cuts, axis=0)

        raw = stacked(queries).astype(F32)
        outs = stacked(out_grad)
        gain = query_gain[...]
        inverse = inverse_of(raw)
        normed = (raw * inverse * gain).astype(BF16)
        keys = gathered[0, sample, :, head].reshape(tokens, head_dim)
        values = gathered[1, sample, :, head].reshape(tokens, head_dim)
        scores = mul(normed, keys, ((1,), (1,))) * scale
        token = lax.broadcasted_iota(jnp.int32, scores.shape, 1)
        scores = jnp.where(token < live, scores, NEG)
        expo = jnp.exp(scores - jnp.max(scores, axis=-1, keepdims=True))
        probs = expo * (1.0 / jnp.sum(expo, axis=-1, keepdims=True))
        probs_b = probs.astype(BF16)
        attn = mul(probs_b, values, ((1,), (0,))).astype(BF16)
        midway()
        delta = jnp.sum(outs.astype(F32) * attn.astype(F32), axis=-1, keepdims=True)
        dprobs = mul(outs, values, ((1,), (1,)))
        dscores = (probs * (dprobs - delta)).astype(BF16)
        value_part = mul(probs_b, outs, ((0,), (0,))).astype(BF16)
        key_part = (mul(dscores, normed, ((0,), (0,))) * scale).astype(BF16)
        parts[0, sample, :, head] = key_part.reshape(n, rows, head_dim)
        parts[1, sample, :, head] = value_part.reshape(n, rows, head_dim)
        dnormed = mul(dscores, keys, ((1,), (0,))) * scale
        back = norm_back(raw, inverse, gain, dnormed).astype(BF16)
        for at in range(group):
            cut = slice(at * head_dim, (at + 1) * head_dim)
            query_out[head, sample, :, cut] = back[at * text_rows : (at + 1) * text_rows]

    def scatter_copy(way, kind, chunk, step, cut, block=None):
        target = held.at[way, kind, chunk, step, cut]
        at = (way, step, kind * samples + chunk, cut)
        block = target if block is None else block
        return remote(block, target, scatter_send.at[0], scatter_recv.at[at], {"seq": ring.nexts[way]})

    def scatter_start(chunk):
        for cut in range(heads):
            for kind in range(2):
                for way in range(2):
                    dest = ring.dest(way, ring.reach(way, kind))
                    scatter_copy(way, kind, chunk, 0, cut, parts.at[kind, chunk, dest, cut]).start()

    def scatter_step(chunk, step, cuts=range(heads), most=None):
        for cut in cuts:
            for kind in range(2):
                for way in range(2):

                    @when(step, ring.reach(way, kind), most)
                    def _():
                        scatter_copy(way, kind, chunk, step - 1, cut).wait_recv()
                        block = held.at[way, kind, chunk, step - 1, cut]
                        dest = ring.dest(way, ring.reach(way, kind) - step)
                        summed = block[...].astype(F32) + parts[kind, chunk, dest, cut].astype(F32)
                        block[...] = summed.astype(BF16)
                        scatter_copy(way, kind, chunk, step, cut, block).start()

    def scatter_sum(kind, chunk, cut):
        total = parts[kind, chunk, here, cut].astype(F32)
        for way in range(2):
            last = ring.reach(way, kind) - 1
            scatter_copy(way, kind, chunk, last, cut).wait_recv()
            total = total + held[way, kind, chunk, last, cut].astype(F32)
        return total

    def scatter_last(chunk):
        gain = key_gain[...]
        for at in range(heads):
            cut = slice(at * head_dim, (at + 1) * head_dim)
            raw = raw_keys[chunk, at]
            summed = scatter_sum(0, chunk, at)
            grads[0, chunk, :, cut] = norm_back(raw, inverse_of(raw), gain, summed).astype(BF16)
            grads[1, chunk, :, cut] = scatter_sum(1, chunk, at).astype(BF16)

    for load in loads[2 + 2 * CUTS :]:
        load.wait()

    early, late = range(heads - heads // 2), range(heads - heads // 2, heads)

    def first_sample(head, carry):
        gather.step(1, head + 1, early, heads)
        push_some(head)
        attend(0, head, lambda: gather.step(1, head + 1, late, heads))
        return carry

    lax.fori_loop(0, heads, first_sample, 0)
    for step in range(heads + 1, reach + 1):
        gather.step(1, step)
    scatter_start(0)

    def second_sample(head, carry):
        scatter_step(0, head + 1, early, heads)
        push_some(heads + head)
        attend(1, head, lambda: scatter_step(0, head + 1, late, heads))
        return carry

    lax.fori_loop(0, heads, second_sample, 0)
    for step in range(heads + 1, reach):
        scatter_step(0, step)
    scatter_start(1)

    row_cuts = row_cuts_of(rows)

    def rows_at(cut):
        return pl.ds(*row_cuts[cut])

    spread = Gather(
        ring,
        pairs,
        samples,
        len(row_cuts),
        lambda kind, chunk, cut: grads.at[kind, chunk, rows_at(cut)],
        lambda kind, chunk, whose, origin, cut: every.at[kind, whose, chunk, origin, rows_at(cut)],
        lambda kind, chunks, count: every.at[kind, 0, :chunks, :count],
        sems[4:8],
    )
    scatter_last(0)
    spread.start(0)
    for step in range(1, reach + 1):
        if step < reach:
            scatter_step(1, step)
        else:
            scatter_last(1)
            spread.start(1)
        spread.step(0, step)
        if step == 1:
            for shift in range(1, pairs * n):
                for copy in pushes(shift):
                    copy.wait_recv()
            for copy in mine_here:
                copy.wait()
            for copy in swaps:
                copy.start()
    for kind in range(2):
        every[kind, lane, :, here] = grads[kind]
    for copy in swaps:
        copy.wait()
    spread.settle(0)

    def product(kind, sample):
        return mul(
            columns[:, sample].reshape(pairs * tokens, shard),
            every[kind, :, sample].reshape(pairs * tokens, model_columns),
            ((0,), (0,)),
        )

    share = total.shape[1]
    tiles = share // tile
    copies = []

    def vision_part(owner, at):
        span = pl.ds(pl.multiple_of(owner * share + at * tile, tile), tile)
        part = None
        for kind in range(2):
            left = grads[kind].reshape(samples * rows, model_columns)
            term = mul(left, weights[kind][span, :], ((1,), (1,)))
            part = term if part is None else part + term
        return part

    def leave(at):
        copy = remote(leaving.at[at], arrived.at[at], leave_sem.at[at], arrive_sem.at[at], {"mp": mates[at]})
        copy.start()
        copies.append(copy)

    jobs = []
    for turn, owner in enumerate(mates + [me]):
        for at in range(tiles):

            def job(turn=turn, owner=owner, at=at):
                span = slice(at * tile, (at + 1) * tile)
                part = vision_part(owner, at)
                if turn == len(mates):
                    total[:, span] = part
                    return
                leaving[turn, :, span] = part.astype(BF16)
                if at == tiles - 1:
                    leave(turn)

            jobs.append(job)

    for kind in range(2):

        def job(kind=kind):
            partial[kind] = product(kind, 0)

        jobs.append(job)
    for step in range(1, reach + 1):
        if step < reach:
            for _ in range(-(-len(jobs) // (reach - step))):
                jobs.pop(0)()
        spread.step(1, step)
    spread.settle(1)

    share_cuts = mine.shape[1]
    cut_rows = shard // share_cuts

    def rows_of(whose, origin, cut):
        return pl.ds(pl.multiple_of(((whose * n + origin) * share_cuts + cut) * cut_rows, cut_rows), cut_rows)

    share_out = Gather(
        ring,
        pairs,
        1,
        share_cuts,
        lambda kind, chunk, cut: mine.at[kind, cut],
        lambda kind, chunk, whose, origin, cut: weights[kind].at[rows_of(whose, origin, cut)],
        lambda kind, chunks, count: weights[kind].at[: count * shard],
        sems[8:],
    )
    for kind in range(2):
        grad = partial[kind]
        for sample in range(1, samples):
            grad = grad + product(kind, sample)
        mine[kind] = grad.astype(BF16).reshape(mine.shape[1:])
        share_out.start(0, (kind,))
    result = total[...]
    for at, copy in enumerate(copies):
        copy.wait()
        result = result + arrived[at].astype(F32)
    vision_out[...] = result.astype(BF16)
    for kind in range(2):
        for cut in range(share_cuts):
            weights[kind][rows_of(lane, here, cut), :] = mine[kind, cut]
    for step in range(1, reach + 1):
        share_out.step(0, step)
    share_out.settle(0)

    for shift in range(1, pairs * n):
        for copy in pushes(shift):
            copy.wait_send()
    sent = parts.at[:, :, : n - 1]
    remote(sent, sent, scatter_send.at[0], scatter_recv.at[0, 0, 0, 0], {"seq": ring.nexts[0]}).wait_send()
    for each in (gather, spread, share_out):
        each.drain()


def emit_kernel(query_ref, vision_ref, key_ref, value_ref, query_out, vision_out, key_out, value_out, staged, sem, own_sem):
    heads, _, _, wide = query_ref.shape
    passed = [pltpu.make_async_copy(vision_ref, vision_out, own_sem.at[heads])]
    for at in range(heads):
        passed.append(
            pltpu.make_async_copy(
                query_ref.at[at], query_out.at[:, :, at * wide : (at + 1) * wide], own_sem.at[at]
            )
        )
    slots, block = staged.shape[:2]
    blocks = key_out.shape[0] // block
    copies = []
    for at in range(2 * blocks):
        kind, span = at // blocks, pl.ds(at % blocks * block, block)
        slot = at % slots
        if at >= slots:
            copies[at - slots].wait()
        staged[slot] = (key_ref, value_ref)[kind][span, :].astype(F32)
        copy = pltpu.make_async_copy(staged.at[slot], (key_out, value_out)[kind].at[span], sem.at[slot])
        copy.start()
        copies.append(copy)
        if at < len(passed):
            passed[at].start()
    for copy in copies[-slots:] + passed:
        copy.wait()


def emit(query_grad, vision_grad, key_grad, value_grad):
    rows, columns = key_grad.shape
    heads, samples, text_rows, wide = query_grad.shape
    grad = jax.ShapeDtypeStruct((rows, columns), F32)
    block = rows // 16
    dma = pltpu.SemaphoreType.DMA
    return pl.pallas_call(
        emit_kernel,
        out_shape=(
            jax.ShapeDtypeStruct((samples, text_rows, heads * wide), BF16),
            jax.ShapeDtypeStruct(vision_grad.shape, BF16),
            grad,
            grad,
        ),
        in_specs=[pl.BlockSpec(memory_space=VMEM)] * 4,
        out_specs=(pl.BlockSpec(memory_space=pltpu.HBM),) * 4,
        scratch_shapes=[VMEM((8, block, columns), F32), dma((8,)), dma((heads + 1,))],
        compiler_params=pltpu.CompilerParams(vmem_limit_bytes=16 * 1024 * 1024),
        cost_estimate=pl.CostEstimate(flops=2 * rows * columns, bytes_accessed=8 * rows * columns, transcendentals=0),
        name="emit",
    )(query_grad, vision_grad, key_grad, value_grad)


def row_cuts_of(rows):
    first = -(-rows // 32) * 16
    return [(0, first), (first, rows - first)] if rows % 16 == 0 and rows > 16 else [(0, rows)]


def ring_sems(n, pairs, chunks, cuts):
    dma = pltpu.SemaphoreType.DMA
    others = max(pairs - 1, 1)
    return [dma((2,)), dma((2, n // 2, 2 * chunks, cuts)), dma((others, 2)), dma((others, chunks, 2))]


def in_hbm(array):
    return pltpu.with_memory_space_constraint(array, pltpu.HBM)


def local(sizes, queries, vision, key_weight, value_weight, query_gain, key_gain, out_grad, tile_count):
    pairs, n, heads_cut = sizes
    samples, rows, width = vision.shape
    columns = key_weight.shape[1]
    head_dim = key_gain.shape[0]
    heads = columns // head_dim
    group = queries.shape[2] // columns
    block = (heads, rows, head_dim)
    by_head = (heads, samples, queries.shape[1], group * head_dim)
    share = width // heads_cut
    shard = width // (pairs * n)
    groups = samples if heads_cut % samples == 0 else 1
    kept = 1 if groups > 1 else samples
    tile = 512 if share % 512 == 0 else share
    share_cuts = 4 if shard % 64 == 0 else 1
    moved = VMEM((max(heads_cut - 1, 1), samples * rows, share), BF16)
    dma = pltpu.SemaphoreType.DMA
    hbm = pl.BlockSpec(memory_space=pltpu.HBM)
    vmem = pl.BlockSpec(memory_space=VMEM)
    sent = 6 * samples * (n - 1) * rows * columns * 2 + 2 * (n - 1) * shard * columns * 2
    whole = pl.pallas_call(
        functools.partial(whole_kernel, sizes, group, n * rows // MAX_TILES, tile),
        out_shape=(
            jax.ShapeDtypeStruct(by_head, BF16),
            jax.ShapeDtypeStruct((samples * rows, share), BF16),
            jax.ShapeDtypeStruct((width, columns), BF16),
            jax.ShapeDtypeStruct((width, columns), BF16),
        ),
        in_specs=[hbm] * 8,
        out_specs=(vmem,) * 4,
        scratch_shapes=[
            VMEM((1, samples), jnp.int32),
            VMEM((1, head_dim), F32),
            VMEM((1, head_dim), F32),
            VMEM(by_head, BF16),
            VMEM(by_head, BF16),
            VMEM(vision.shape, BF16),
            VMEM((2, samples, *block), BF16),
            VMEM((samples, *block), F32),
            VMEM((2, samples, n, *block), BF16),
            VMEM((2, samples, n, *block), BF16),
            VMEM((2, 2, samples, n // 2, *block), BF16),
            VMEM((pairs, samples, n, rows, shard), BF16),
            VMEM((2, samples, rows, columns), BF16),
            moved,
            moved,
            VMEM((samples * rows, share), F32),
            VMEM((2, pairs, samples, n, rows, columns), BF16),
            VMEM((2, share_cuts, shard // share_cuts, columns), BF16),
            VMEM((2, shard, columns), F32),
            dma((4 + 2 * CUTS + 2 * heads,)),
            dma((kept,)),
            dma((kept, pairs * n)),
            dma((kept, pairs * n)),
            dma((pairs, max(groups - 1, 1))),
            dma((pairs, max(groups - 1, 1))),
            dma((1,)),
            dma((2, n // 2, 2 * samples, heads)),
            dma((max(heads_cut - 1, 1),)),
            dma((max(heads_cut - 1, 1),)),
        ]
        + ring_sems(n, 1, samples, heads)
        + ring_sems(n, pairs, samples, len(row_cuts_of(rows)))
        + ring_sems(n, pairs, 1, share_cuts),
        compiler_params=pltpu.CompilerParams(
            collective_id=1, has_side_effects=True, vmem_limit_bytes=LIMIT
        ),
        cost_estimate=pl.CostEstimate(flops=25_000_000_000, bytes_accessed=sent, transcendentals=0),
        name="whole",
    )(
        *map(
            in_hbm,
            (
                tile_count[None],
                queries,
                vision,
                key_weight,
                value_weight,
                query_gain[None],
                key_gain[None],
                out_grad,
            ),
        )
    )
    query_grad, vision_grad, key_grad, value_grad = emit(*whole)
    return query_grad, vision_grad.reshape(samples, rows, share), key_grad, value_grad


LIMIT = 38 * 1024 * 1024


def solution(mesh):
    sizes = (mesh.shape["dp"], mesh.shape["seq"], mesh.shape["mp"])
    in_specs = (
        P("dp", "seq", "mp"),
        P("dp", "seq", None),
        P(None, "mp"),
        P(None, "mp"),
        P(),
        P(),
        P("dp", "seq", "mp"),
        P("dp"),
    )
    out_specs = (P("dp", "seq", "mp"), P("dp", "seq", "mp"), P(None, "mp"), P(None, "mp"))
    return jax.shard_map(
        functools.partial(local, sizes), mesh=mesh, in_specs=in_specs, out_specs=out_specs, check_vma=False
    )
```
